128 devices in a mesh: grp: 16 (over z, x_lo, core), blk: 8 (over x_hi, y).
Axes of the slice: x: 4 (x_hi: 2, x_lo: 2; x = x_hi * 2 + x_lo), y: 4, z: 4, core: 2. Of those that a mesh axis runs over, the one named last changes fastest.
Arguments:
- temp: float32 [8, 1024, 1024], P(None, 'grp', 'blk'), may hold values from -6 to 6
- uvel: float32 [8, 1024, 1024], P(None, 'grp', 'blk'), may hold values from -0.4 to 0.4
- vvel: float32 [8, 1024, 1024], P(None, 'grp', 'blk'), may hold values from -0.4 to 0.4
- couple_col: int32 [16, 8, 2048], P('grp', 'blk'), may hold values from 0 to 8191
- couple_cell: int32 [16, 8, 2048], P('grp', 'blk'), may hold values from 0 to 1048575
- cavity: int32 [16, 8, 2048], P('grp', 'blk'), may hold values 0 or 1
- thickness: float32 [1024, 1024], P('blk'), may hold values from 0.2 to 2
- viscosity: float32 [1024, 1024], P('blk'), may hold values from 0.5 to 4
- friction: float32 [1024, 1024], P('blk'), may hold values from 0.02 to 0.3
- drive: float32 [1024, 1024], P('blk'), may hold values from -6 to 6
Outputs:
- temp_new: float32 [8, 1024, 1024], P(None, 'grp', 'blk')
- ice_velocity: float32 [1024, 1024], P('blk')
The draws below stay inside these ranges and needn't reach their ends.
Inputs may be any that keep to these rules, and one draw needn't show every extreme that they name: `couple_col`: an index of a column within the 64 x 128 block of the device holding the entry, row-major. `couple_cell`: a row-major index into the whole ice grid.
All inputs are finite; a program needn't handle non-finite values. No bound on the sum of `cavity` on one device may be relied on, other than what follows from the above.
Results may differ from the reference program's by a relative error of at most 0.0003.
Values sent between devices are 32-bit elements; how exact they have to be, the bound alone decides.
No kernel may reach another device: no remote copies, remote signals or barrier semaphores. Data moves between devices by JAX's collectives and lax.ppermute only.
A program may use at most 64 MiB of HBM per device.

```python
import math
import jax
import jax.numpy as jnp
from jax import lax

LEV = 8
CX = 64
CY = 128
CIX = 128
IY = 1024
COUPLE = 2048
LEVELS = 3
SMOOTH_SWEEPS = 2
COARSE_SWEEPS = 4
CYCLES = 2
OX = 1024
OY = 1024
NIX = 1024
NI = 1048576
N_GRP = 16
N_BLK = 8


def touch_ends(entries, rng, least, top_value):
    spot = [jax.random.randint(jax.random.fold_in(rng, axis), (), 0, length) for axis, length in enumerate(entries.shape)]
    longest = entries.shape.index(max(entries.shape))
    neighbour = spot[:longest] + [(spot[longest] + 1) % entries.shape[longest]] + spot[longest + 1:]
    return entries.at[tuple(spot)].set(least).at[tuple(neighbour)].set(top_value)


def level_of(key, extent, cuts, smallest, high):
    level = 1.0
    for dim, parts in cuts:
        steps = jax.random.uniform(jax.random.fold_in(jax.random.fold_in(key, 6), dim), (parts,), jnp.float32, smallest / len(cuts), high / len(cuts))
        level = level * jnp.repeat(jnp.exp(steps), extent[dim] // parts).reshape((-1,) + (1,) * (len(extent) - 1 - dim))
    return level


def bell_draw(own_key, dims, deviation, most, pieces=(), kind=jnp.bfloat16):
    entries = deviation * jax.random.normal(own_key, dims, jnp.float32)
    if pieces:
        entries = entries * level_of(own_key, dims, pieces, -0.22, 0.18)
    return jnp.clip(entries, -most, most).astype(kind)


def setup_inputs(seed: int = 0) -> dict:
    keys = jax.random.split(jax.random.key(seed), 11)
    return {
        "temp": bell_draw(keys[0], (LEV, OX, OY), 1.0, 6.0, ((1, 16), (2, 8)), jnp.float32),
        "uvel": jnp.clip(jax.random.uniform(keys[1], (LEV, OX, OY), jnp.float32, -0.4, 0.4) * level_of(keys[1], (LEV, OX, OY), ((1, 16), (2, 8)), -0.4, 0.0), -0.4, 0.4),
        "vvel": jnp.clip(jax.random.uniform(keys[2], (LEV, OX, OY), jnp.float32, -0.4, 0.4) * level_of(keys[2], (LEV, OX, OY), ((1, 16), (2, 8)), -0.4, 0.0), -0.4, 0.4),
        "couple_col": touch_ends(jax.random.randint(keys[3], (N_GRP, N_BLK, COUPLE), 0, CX * CY), jax.random.fold_in(keys[3], 1), 0, (CX * CY) - 1).astype(jnp.int32),
        "couple_cell": touch_ends(jax.random.randint(keys[4], (N_GRP, N_BLK, COUPLE), 0, NI), jax.random.fold_in(keys[4], 1), 0, NI - 1).astype(jnp.int32),
        "cavity": touch_ends((jax.random.randint(keys[5], (N_GRP, N_BLK, COUPLE), 0, 2) < 1).astype(jnp.int32), jax.random.fold_in(keys[5], 1), 0, 1),
        "thickness": jnp.clip(0.2 + 1.8 * jax.random.uniform(keys[6], (NIX, IY), jnp.float32) ** level_of(keys[6], (NIX, IY), ((0, 8),), -0.2, 0.2), 0.2, 2.0),
        "viscosity": jnp.clip(jnp.exp(math.log(4.0) - 2.0794415 * jax.random.uniform(keys[7], (NIX, IY), jnp.float32) ** level_of(keys[7], (NIX, IY), ((0, 8),), -0.2, 0.2)), 0.5, 4.0),
        "friction": jnp.clip(jnp.exp(math.log(0.3) - 2.7080503 * jax.random.uniform(keys[8], (NIX, IY), jnp.float32) ** level_of(keys[8], (NIX, IY), ((0, 8),), -0.2, 0.2)), 0.02, 0.3),
        "drive": bell_draw(keys[9], (NIX, IY), 1.0, 6.0, ((0, 8),), jnp.float32),
    }


omega = 0.8
kappa = 0.1
vertical_mix = 0.2
melt_rate = 0.5


def face_terms(visc_pad, friction, scale):
    center = visc_pad[1:-1, 1:-1]
    east = 0.5 * (center + visc_pad[2:, 1:-1]) * scale
    west = 0.5 * (center + visc_pad[:-2, 1:-1]) * scale
    north = 0.5 * (center + visc_pad[1:-1, 2:]) * scale
    south = 0.5 * (center + visc_pad[1:-1, :-2]) * scale
    diagonal = east + west + north + south + friction
    return (east, west, north, south, diagonal)


def apply_padded(field_pad, terms):
    east, west, north, south, diagonal = terms
    field = field_pad[1:-1, 1:-1]
    return (diagonal * field - east * field_pad[2:, 1:-1] - west * field_pad[:-2, 1:-1]
            - north * field_pad[1:-1, 2:] - south * field_pad[1:-1, :-2])


def restrict(field):
    paired = field[0::2] + field[1::2]
    return 0.25 * (paired[:, 0::2] + paired[:, 1::2])


def prolong(field):
    rows, cols = field.shape
    expand = (jnp.arange(2 * cols)[None, :] // 2 == jnp.arange(cols)[:, None]).astype(jnp.float32)
    wide = jnp.dot(field, expand, precision=lax.Precision.HIGHEST)
    return jnp.broadcast_to(wide[:, None, :], (rows, 2, 2 * cols)).reshape(2 * rows, 2 * cols)


def vcycle(depth, field, source, terms_list, operate):
    terms = terms_list[depth]
    sweeps = COARSE_SWEEPS if depth == LEVELS - 1 else SMOOTH_SWEEPS
    for sweep_index in range(sweeps):
        field = field + omega * (source - operate(field, terms)) / terms[4]
    if depth == LEVELS - 1:
        return field
    residual = source - operate(field, terms)
    coarse_source = restrict(residual)
    coarse = vcycle(depth + 1, jnp.zeros_like(coarse_source), coarse_source, terms_list, operate)
    field = field + prolong(coarse)
    for sweep_index in range(SMOOTH_SWEEPS):
        field = field + omega * (source - operate(field, terms)) / terms[4]
    return field


def ocean_tendency(temp_pad, uvel_pad, vvel_pad):
    temp = temp_pad[:, 1:-1, 1:-1]
    uvel = uvel_pad[:, 1:-1, 1:-1]
    vvel = vvel_pad[:, 1:-1, 1:-1]
    east_speed = 0.5 * (uvel + uvel_pad[:, 2:, 1:-1])
    flux_east = jnp.maximum(east_speed, 0.0) * temp + jnp.minimum(east_speed, 0.0) * temp_pad[:, 2:, 1:-1]
    west_speed = 0.5 * (uvel + uvel_pad[:, :-2, 1:-1])
    flux_west = jnp.maximum(west_speed, 0.0) * temp_pad[:, :-2, 1:-1] + jnp.minimum(west_speed, 0.0) * temp
    north_speed = 0.5 * (vvel + vvel_pad[:, 1:-1, 2:])
    flux_north = jnp.maximum(north_speed, 0.0) * temp + jnp.minimum(north_speed, 0.0) * temp_pad[:, 1:-1, 2:]
    south_speed = 0.5 * (vvel + vvel_pad[:, 1:-1, :-2])
    flux_south = jnp.maximum(south_speed, 0.0) * temp_pad[:, 1:-1, :-2] + jnp.minimum(south_speed, 0.0) * temp
    laplace = (temp_pad[:, 2:, 1:-1] + temp_pad[:, :-2, 1:-1] + temp_pad[:, 1:-1, 2:]
               + temp_pad[:, 1:-1, :-2] - 4.0 * temp)
    between = temp[1:] - temp[:-1]
    zero_layer = jnp.zeros_like(temp[:1])
    vert = jnp.concatenate([between, zero_layer], axis=0) - jnp.concatenate([zero_layer, between], axis=0)
    return temp + flux_west - flux_east + flux_south - flux_north + kappa * laplace + vertical_mix * vert


def operate_whole(field, terms):
    return apply_padded(jnp.pad(field, 1), terms)


def reference(temp, uvel, vvel, couple_col, couple_cell, cavity, thickness, viscosity, friction, drive):
    blocks = N_GRP * N_BLK
    top = temp[0].reshape(N_GRP, CX, N_BLK, CY).transpose(0, 2, 1, 3).reshape(blocks, CX * CY)
    columns = couple_col.reshape(blocks, COUPLE)
    cells = couple_cell.reshape(-1)
    top_entry = jnp.take_along_axis(top, columns, axis=1).reshape(-1)
    draft = thickness.reshape(-1)[cells]
    melt = cavity.reshape(-1).astype(jnp.float32) * melt_rate * (top_entry + 0.5 + 0.5 * draft)

    def column_sum(values, positions):
        return jax.ops.segment_sum(values, positions, CX * CY)

    column_melt = jax.vmap(column_sum)(melt.reshape(blocks, COUPLE), columns)
    surface = column_melt.reshape(N_GRP, N_BLK, CX, CY).transpose(0, 2, 1, 3).reshape(N_GRP * CX, N_BLK * CY)
    padded = jnp.pad(jnp.stack([temp, uvel, vvel]), ((0, 0), (0, 0), (1, 1), (1, 1)))
    stepped = ocean_tendency(padded[0], padded[1], padded[2])
    temp_new = jnp.concatenate([stepped[:1] - melt_rate * surface[None], stepped[1:]], axis=0)

    melt_ice = jax.ops.segment_sum(melt, cells, N_BLK * CIX * IY).reshape(N_BLK * CIX, IY)
    source = drive + melt_ice
    terms_list = []
    visc = viscosity
    fric = friction
    for depth in range(LEVELS):
        terms_list.append(face_terms(jnp.pad(visc, 1), fric, 0.25 ** depth))
        if depth + 1 < LEVELS:
            visc = restrict(visc)
            fric = restrict(fric)
    field = jnp.zeros_like(source)
    for cycle_index in range(CYCLES):
        field = vcycle(0, field, source, terms_list, operate_whole)
    return temp_new, field
```

```python
import functools
import jax
import jax.numpy as jnp
from jax import lax
from jax.experimental import pallas as pl
from jax.experimental.pallas import tpu as pltpu
from jax.sharding import Mesh
from jax.sharding import PartitionSpec as P

LEVELS = 3
CYCLES = 2
GRP = ("z", "xl", "co")
ZX = ("z", "xl")
BLK = ("xh", "y")
omega = 0.8
kappa = 0.1
vertical_mix = 0.2
melt_rate = 0.5

LEV = 8
CX = 64
CY = 128
ROWS = 128
COLS = 1024
HALF = 64
ENT = 2048
EXT = 192
KC = 512
N_BLK = 8
CELLS = ROWS * COLS
f32 = jnp.float32
bf16 = jnp.bfloat16
i32 = jnp.int32
VMEM = pl.BlockSpec(memory_space=pltpu.VMEM)
SMEM = pl.BlockSpec(memory_space=pltpu.SMEM)


def split2(x):
    high = x.astype(bf16)
    low = (x - high.astype(f32)).astype(bf16)
    return high, low


def split3(x):
    high = x.astype(bf16)
    rest = x - high.astype(f32)
    mid = rest.astype(bf16)
    return high, mid, (rest - mid.astype(f32)).astype(bf16)


def sub_iota(shape):
    return lax.broadcasted_iota(i32, shape, 0)


def lane_iota(shape):
    return lax.broadcasted_iota(i32, shape, 1)


NT = (((1,), (1,)), ((), ()))


def pack_kernel(temp, uvel, vvel, col, cell, cav, packet, row_lo, row_hi, col_lo, col_hi):
    tops = split3(temp[0].T)
    table = jnp.concatenate(tops, axis=0)
    for j in range(ENT // KC):
        c = col[0, :, j * KC : (j + 1) * KC]
        rows = jnp.where(sub_iota((CX, KC)) == (c >> 7), 1.0, 0.0).astype(bf16)
        picked = jnp.dot(table, rows, preferred_element_type=f32)
        picked = picked[0:128] + picked[128:256] + picked[256:384]
        mask = sub_iota((CY, KC)) == (c & 127)
        top = jnp.sum(jnp.where(mask, picked, 0.0), axis=0, keepdims=True)
        on = cav[0, :, j * KC : (j + 1) * KC] > 0
        index = jnp.where(on, cell[0, :, j * KC : (j + 1) * KC], -1)
        packet[0:1, j * KC : (j + 1) * KC] = index.astype(f32)
        packet[1:2, j * KC : (j + 1) * KC] = top
    for k in range(LEV):
        row_lo[k : k + 1, :] = temp[k, 0:1, :]
        row_lo[k + 8 : k + 9, :] = uvel[k, 0:1, :]
        row_hi[k : k + 1, :] = temp[k, CX - 1 : CX, :]
        row_hi[k + 8 : k + 9, :] = uvel[k, CX - 1 : CX, :]
        across = temp[k].T
        col_lo[k : k + 1, :] = across[0:1, :]
        col_hi[k : k + 1, :] = across[CY - 1 : CY, :]
        across = vvel[k].T
        col_lo[k + 8 : k + 9, :] = across[0:1, :]
        col_hi[k + 8 : k + 9, :] = across[CY - 1 : CY, :]


def pack(temp, uvel, vvel, col, cell, cav):
    return pl.pallas_call(
        pack_kernel,
        out_shape=(
            jax.ShapeDtypeStruct((2, ENT), f32),
            jax.ShapeDtypeStruct((16, CY), f32),
            jax.ShapeDtypeStruct((16, CY), f32),
            jax.ShapeDtypeStruct((16, CX), f32),
            jax.ShapeDtypeStruct((16, CX), f32),
        ),
        in_specs=[VMEM] * 6,
        out_specs=(VMEM,) * 5,
        name="pack",
    )(temp, uvel, vvel, col, cell, cav)


def place(packets, first, k):
    at = pl.multiple_of((k % (ENT // KC)) * KC, KC)
    index = packets[k // (ENT // KC), 0:1, pl.ds(at, KC)].astype(i32)
    local = index - first
    row = local >> 10
    spot = ((row >> 3) << 6) | (((local >> 7) & 7) << 3) | (row & 7)
    spot = jnp.where((local >= 0) & (local < CELLS), spot, -1)
    return spot, local & 127, at


def scatter_kernel(where, packets, thick, mine, other, onehot, lanes, acc, melt):
    first, core = where[0], where[1]
    acc[...] = jnp.zeros_like(acc)

    def chunk(k, carry):
        spot, lane, at = place(packets, first, k)
        top = packets[k // (ENT // KC), 1:2, pl.ds(at, KC)]
        high = top.astype(bf16).astype(f32)
        onehot[...] = jnp.where(sub_iota((1024, KC)) == spot, 1.0, 0.0).astype(bf16)
        mask = sub_iota((128, KC)) == lane
        lanes[0:128, :] = jnp.where(mask, high, 0.0).astype(bf16)
        lanes[128:256, :] = jnp.where(mask, top - high, 0.0).astype(bf16)
        lanes[256:384, :] = jnp.where(mask, 1.0, 0.0).astype(bf16)
        acc[...] += lax.dot_general(onehot[...], lanes[...], NT, preferred_element_type=f32)
        return carry

    lax.fori_loop(0, N_BLK * ENT // KC, chunk, 0)
    for t in range(128):
        i, c = t // 8, t % 8
        rows = slice(t * 8, t * 8 + 8)
        heat = acc[rows, 0:128] + acc[rows, 128:256]
        draft = thick[i * 8 : i * 8 + 8, c * 128 : c * 128 + 128]
        value = 0.5 * heat + (0.25 + 0.25 * draft) * acc[rows, 256:384]
        melt[i // 8, (i % 8) * 8 : (i % 8) * 8 + 8, c * 128 : c * 128 + 128] = value
    mine[...] = melt[core]
    other[...] = melt[1 - core]


def scatter(where, packets, thick):
    half = jax.ShapeDtypeStruct((HALF, COLS), f32)
    return pl.pallas_call(
        scatter_kernel,
        out_shape=(half, half),
        in_specs=[SMEM, VMEM, VMEM],
        out_specs=(VMEM, VMEM),
        scratch_shapes=[
            pltpu.VMEM((1024, KC), bf16),
            pltpu.VMEM((384, KC), bf16),
            pltpu.VMEM((1024, 384), f32),
            pltpu.VMEM((2, HALF, COLS), f32),
        ],
        name="scatter",
    )(where, packets, thick)


def draft_kernel(where, packets, thick, near, far, tiles, table, onehot):
    first = where[0]
    for t in range(128):
        i, c = t // 8, t % 8
        tiles[t * 8 : t * 8 + 8, :] = thick[i * 8 : i * 8 + 8, c * 128 : c * 128 + 128]
    for a in range(8):
        high, low = split2(tiles[a * 128 : a * 128 + 128, :].T)
        table[0:128, a * 128 : a * 128 + 128] = high
        table[128:256, a * 128 : a * 128 + 128] = low

    def chunk(k, out):
        spot, lane, at = place(packets, first, k)
        onehot[...] = jnp.where(sub_iota((1024, KC)) == spot, 1.0, 0.0).astype(bf16)
        picked = jnp.dot(table[...], onehot[...], preferred_element_type=f32)
        picked = picked[0:128] + picked[128:256]
        mask = sub_iota((128, KC)) == lane
        found = jnp.sum(jnp.where(mask, picked, 0.0), axis=0, keepdims=True)
        s = k // (ENT // KC)
        out[s % 4, 0:1, pl.ds(at, KC)] = found

    per = 4 * ENT // KC

    def low_chunk(k, carry):
        chunk(k, near)
        return carry

    def high_chunk(k, carry):
        chunk(k, far)
        return carry

    lax.fori_loop(per, 2 * per, high_chunk, 0)
    lax.fori_loop(0, per, low_chunk, 0)


def drafts(where, packets, thick):
    out = jax.ShapeDtypeStruct((4, 1, ENT), f32)
    return pl.pallas_call(
        draft_kernel,
        out_shape=(out, out),
        in_specs=[SMEM, VMEM, VMEM],
        out_specs=(VMEM, VMEM),
        scratch_shapes=[
            pltpu.VMEM((1024, 128), f32),
            pltpu.VMEM((256, 1024), bf16),
            pltpu.VMEM((1024, KC), bf16),
        ],
        name="drafts",
    )(where, packets, thick)


def ocean_kernel(
    temp, uvel, vvel, below, above, west, east, col, cav, packet, d0, d1, d2, d3, d4, out
):
    shape = (CX, CY)
    row, lane = sub_iota(shape), lane_iota(shape)
    heat = jnp.zeros((CX, 384), f32)
    for j in range(ENT // KC):
        at = slice(j * KC, (j + 1) * KC)
        draft = d0[0, :, at] + d1[0, :, at] + d2[0, :, at] + d3[0, :, at] + d4[0, :, at]
        c = col[0, :, at]
        melt = cav[0, :, at].astype(f32) * melt_rate * (packet[1:2, at] + 0.5 + 0.5 * draft)
        rows = jnp.where(sub_iota((CX, KC)) == (c >> 7), 1.0, 0.0).astype(bf16)
        mask = sub_iota((CY, KC)) == (c & 127)
        parts = [
            jnp.where(mask, part.astype(f32), 0.0).astype(bf16) for part in split3(melt)
        ]
        weights = jnp.concatenate(parts, axis=0)
        heat += lax.dot_general(rows, weights, NT, preferred_element_type=f32)
    column_melt = heat[:, 0:128] + heat[:, 128:256] + heat[:, 256:384]
    west_t, east_t = west[...].T, east[...].T

    def nearby(field, k, side):
        x = field[k]
        e = jnp.where(row == CX - 1, above[side + k : side + k + 1, :], pltpu.roll(x, CX - 1, 0))
        w = jnp.where(row == 0, below[side + k : side + k + 1, :], pltpu.roll(x, 1, 0))
        return x, e, w

    def beside(field, k, side):
        x = field[k]
        n = jnp.where(lane == CY - 1, east_t[:, side + k : side + k + 1], pltpu.roll(x, CY - 1, 1))
        s = jnp.where(lane == 0, west_t[:, side + k : side + k + 1], pltpu.roll(x, 1, 1))
        return x, n, s

    for k in range(LEV):
        t, te, tw = nearby(temp, k, 0)
        _, tn, ts = beside(temp, k, 0)
        u, ue, uw = nearby(uvel, k, 8)
        v, vn, vs = beside(vvel, k, 8)
        speed = 0.5 * (u + ue)
        flux_east = jnp.maximum(speed, 0.0) * t + jnp.minimum(speed, 0.0) * te
        speed = 0.5 * (u + uw)
        flux_west = jnp.maximum(speed, 0.0) * tw + jnp.minimum(speed, 0.0) * t
        speed = 0.5 * (v + vn)
        flux_north = jnp.maximum(speed, 0.0) * t + jnp.minimum(speed, 0.0) * tn
        speed = 0.5 * (v + vs)
        flux_south = jnp.maximum(speed, 0.0) * ts + jnp.minimum(speed, 0.0) * t
        laplace = te + tw + tn + ts - 4.0 * t
        lower = temp[k + 1] - t if k + 1 < LEV else 0.0
        upper = t - temp[k - 1] if k else 0.0
        new = t + flux_west - flux_east + flux_south - flux_north
        new = new + kappa * laplace + vertical_mix * (lower - upper)
        out[k] = new - melt_rate * column_melt if k == 0 else new


def ocean(*arrays):
    return pl.pallas_call(
        ocean_kernel,
        out_shape=jax.ShapeDtypeStruct((LEV, CX, CY), f32),
        in_specs=[VMEM] * len(arrays),
        out_specs=VMEM,
        name="ocean",
    )(*arrays)


UP, DOWN, LEFT, RIGHT, INV, SCALE, G = range(7)


def solve_kernel(where, own, partner, near, visc, fric, drive, edge, out, *scratch):
    (vx, fx, sx, k0, k1, k2, v0, v1, v2, f1, f2, g2, res0, res1) = scratch
    core, base = where[1], where[2]
    zero8 = jnp.zeros((8, COLS), f32)

    def put(ref, rows, value):
        if len(ref.shape) == 2:
            ref[rows, :] = value
        else:
            for c in range(8):
                ref[c, rows, :] = value[:, c * 128 : c * 128 + 128]

    def take(ref, rows):
        if len(ref.shape) == 2:
            return ref[rows, :]
        return jnp.concatenate([ref[c, rows, :] for c in range(8)], axis=1)

    for ref in (vx, fx, sx):
        put(ref, slice(0, 8), zero8)
        put(ref, slice(EXT + 8, EXT + 16), zero8)

    for n, (block, full) in enumerate(((visc, vx), (fric, fx), (drive, sx))):

        @pl.when(core == 0)
        def _(n=n, block=block, full=full):
            put(full, slice(8, 72), edge[n])
            put(full, slice(72, 200), block[...])

        @pl.when(core == 1)
        def _(n=n, block=block, full=full):
            put(full, slice(8, 136), block[...])
            put(full, slice(136, 200), edge[n])

    sx[72:136, :] += own[...]

    @pl.when(core == 0)
    def _():
        sx[8:72, :] += near[...]
        sx[136:200, :] += partner[...]

    @pl.when(core == 1)
    def _():
        sx[8:72, :] += partner[...]
        sx[136:200, :] += near[...]

    lane = lane_iota((8, COLS))
    rowi = sub_iota((8, COLS))
    tiles = [EXT // 8 >> level for level in range(LEVELS)]
    ks = (k0, k1, k2)
    vs = (v0, v1, v2)

    def tile(i, d=1):
        if isinstance(i, int):
            return slice(8 * i + 8 * d, 8 * i + 8 * d + 8)
        return pl.ds(pl.multiple_of(8 * i + 8 * d, 8), 8)

    def shifted(ref, i):
        x = take(ref, tile(i))
        above = jnp.where(rowi == 7, take(ref, tile(i, 0)), x)
        below = jnp.where(rowi == 0, take(ref, tile(i, 2)), x)
        return pltpu.roll(above, 1, 0), pltpu.roll(below, 7, 0)

    def loop(lo, hi, body):
        def step(i, carry):
            body(i)
            return carry

        lax.fori_loop(lo, hi, step, 0)

    def left_of(x, s):
        return pltpu.roll(x, s, 1)

    def right_of(x, s):
        return pltpu.roll(x, COLS - s, 1)

    def halved(ref, i, s):
        def at(d):
            return take(ref, pl.ds(16 * i + 8 + d, 8, stride=2))

        pair = at(0) + at(1)
        beside = jnp.where((lane & s) == 0, right_of(pair, s), left_of(pair, s))
        return 0.25 * (pair + beside)

    viscs, frics = (vx, f1, f2), (fx, res1, g2)
    for level in range(LEVELS):
        s = 1 << level
        n = tiles[level]
        kr, vr, fr = ks[level], viscs[level], frics[level]
        if level:

            def coarsen(i, level=level, vr=vr, fr=fr, s=s):
                put(vr, tile(i), halved(viscs[level - 1], i, s // 2))
                put(fr, tile(i), halved(frics[level - 1], i, s // 2))

            put(vr, slice(0, 8), zero8)
            put(vr, slice(n * 8 + 8, n * 8 + 16), zero8)
            for i in range(n):
                coarsen(i)
        scale = 0.5 * 0.25**level
        start = base >> level

        def coefficients(i, level=level, kr=kr, vr=vr, fr=fr, s=s, scale=scale, start=start):
            x = take(vr, tile(i))
            above, below = shifted(vr, i)
            cu = scale * (x + above)
            cd = scale * (x + below)
            cl = scale * (x + jnp.where(lane < s, 0.0, left_of(x, s)))
            cr = scale * (x + jnp.where(lane >= COLS - s, 0.0, right_of(x, s)))
            diag = cu + cd + cl + cr + take(fr, tile(i))
            row = start + 8 * i + rowi
            inside = (row >= 0) & (row < (COLS >> level))
            inv = jnp.where(inside, omega / diag, 0.0)
            kr[UP, tile(i), :] = inv * cu
            kr[DOWN, tile(i), :] = inv * cd
            kr[LEFT, tile(i), :] = jnp.where(lane < s, 0.0, inv * cl)
            kr[RIGHT, tile(i), :] = jnp.where(lane >= COLS - s, 0.0, inv * cr)
            kr[SCALE, tile(i), :] = jnp.where(inside, diag * (1.0 / omega), 0.0)
            kr[INV, tile(i), :] = inv
            if level == 0:
                kr[G, tile(i), :] = inv * sx[tile(i), :]

        loop(0, n, coefficients)

    def step_of(level, src, i):
        kr, s = ks[level], 1 << level
        v = src[tile(i), :]
        above, below = shifted(src, i)
        total = kr[G, tile(i), :] + kr[UP, tile(i), :] * above + kr[DOWN, tile(i), :] * below
        total = total + kr[LEFT, tile(i), :] * left_of(v, s)
        total = total + kr[RIGHT, tile(i), :] * right_of(v, s)
        return v, total - omega * v

    def core_tiles(level, h):
        n = tiles[level]
        return max(n // 3 - h, 0), min(2 * n // 3 + h, n)

    def sweep(level, a, b, h):
        src, dst = vs[level].at[a], vs[level].at[b]

        def body(i):
            v, t = step_of(level, src, i)
            dst[tile(i), :] = v + t

        loop(*core_tiles(level, h), body)

    def residual(level, a, h, res):
        src = vs[level].at[a]

        def body(i):
            _, t = step_of(level, src, i)
            put(res, tile(i), t * ks[level][SCALE, tile(i), :])

        loop(*core_tiles(level, h), body)

    def free_sweep(level, a, h, source, s):
        kr, dst = ks[level], vs[level].at[a]

        def body(i):
            if source is not None:
                kr[G, tile(i), :] = kr[INV, tile(i), :] * halved(source, i, s)
            dst[tile(i), :] = kr[G, tile(i), :]

        if source is None:
            loop(*core_tiles(level, h), body)
            return
        for i in range(*core_tiles(level, h)):
            body(i)

    def correct(level, a, b, h, spread):
        fine, coarse = vs[level].at[a], vs[level + 1].at[b]
        lo, hi = core_tiles(level, h)

        def widen(i):
            e = coarse[tile(i), :]
            put(spread, pl.ds(16 * i + 8, 8, stride=2), e)
            put(spread, pl.ds(16 * i + 9, 8, stride=2), e)

        for i in range(lo // 2, (hi + 1) // 2):
            widen(i)

        def add(i):
            fine[tile(i), :] += take(spread, tile(i))

        loop(lo, hi, add)

    def clear(ref, i):
        put(ref, tile(i, 0), zero8)

    for level in range(LEVELS):
        for a in range(2):
            loop(0, tiles[level] + 2, functools.partial(clear, vs[level].at[a]))
    loop(0, tiles[0] + 2, functools.partial(clear, res0))
    loop(0, tiles[1] + 2, functools.partial(clear, res1))

    for cycle in range(CYCLES):
        first = cycle == 0
        now = 1
        if first:
            free_sweep(0, 0, 8, None, 1)
        else:
            sweep(0, 1, 0, 4)
        sweep(0, 0, 1, 8 if first else 4)
        residual(0, now, 7 if first else 4, res0)
        free_sweep(1, 0, 4 if first else 2, res0, 1)
        sweep(1, 0, 1, 4 if first else 2)
        residual(1, 1, 3 if first else 2, res1)
        h2 = 2 if first else 1
        free_sweep(2, 0, h2, res1, 2)
        sweep(2, 0, 1, h2)
        sweep(2, 1, 0, h2)
        sweep(2, 0, 1, h2)
        correct(1, 1, 1, 3 if first else 1, f1)
        sweep(1, 1, 0, 3 if first else 1)
        sweep(1, 0, 1, 3 if first else 1)
        correct(0, now, 1, 4 if first else 1, vx)
        sweep(0, now, 1 - now, 4 if first else 1)
        sweep(0, 1 - now, now, 4 if first else 0)
    out[...] = v0[1, 72:136, :]


def solve(where, own, partner, near, visc, fric, drive, edge):
    def rows(level, *lead):
        return pltpu.VMEM((*lead, (EXT >> level) + 16, COLS), f32)

    def blocks(level):
        return pltpu.VMEM((8, (EXT >> level) + 16, 128), f32)

    return pl.pallas_call(
        solve_kernel,
        out_shape=jax.ShapeDtypeStruct((HALF, COLS), f32),
        in_specs=[SMEM] + [VMEM] * 7,
        out_specs=VMEM,
        scratch_shapes=[
            blocks(0),
            blocks(0),
            rows(0),
            rows(0, 7),
            rows(1, 7),
            rows(2, 7),
            rows(0, 2),
            rows(1, 2),
            rows(2, 2),
            blocks(1),
            rows(2),
            rows(2),
            blocks(0),
            blocks(1),
        ],
        name="solve",
    )(where, own, partner, near, visc, fric, drive, edge)


def flip(n, k):
    return [(i, i ^ k) for i in range(n)]


def chain(n, d):
    return [(i, i + d) for i in range(n) if 0 <= i + d < n]


def shards(temp, uvel, vvel, col, cell, cav, thick, visc, fric, drive):
    core = lax.axis_index("co").astype(i32)
    blk = lax.axis_index("xh").astype(i32) * 4 + lax.axis_index("y").astype(i32)
    where = jnp.stack([blk * CELLS, core, blk * ROWS + core * HALF - 64])

    packet, row_lo, row_hi, col_lo, col_hi = pack(temp, uvel, vvel, col, cell, cav)
    got = [packet] + [lax.ppermute(packet, "y", flip(4, k)) for k in range(1, 4)]
    got = jnp.stack(got)
    packets = jnp.concatenate([got, lax.ppermute(got, "xh", flip(2, 1))], axis=0)

    ring = ("co", "xh", "y")
    outer = [(b, 8 + b - 1) for b in range(1, 8)] + [(8 + b, b + 1) for b in range(7)]
    ice = jnp.stack([visc, fric, drive])
    ice_edge = lax.dynamic_slice_in_dim(ice, core * HALF, HALF, axis=1)
    edge = lax.ppermute(ice_edge, ring, outer)

    below = lax.ppermute(row_hi, GRP, chain(16, 1))
    above = lax.ppermute(row_lo, GRP, chain(16, -1))
    west = lax.ppermute(col_hi, BLK, chain(8, 1))
    east = lax.ppermute(col_lo, BLK, chain(8, -1))

    mine, other = scatter(where, packets, thick)
    mine = mine + lax.ppermute(other, "co", flip(2, 1))
    parts = lax.all_to_all(mine.reshape(8, 8, COLS), ZX, 0, 0, tiled=True)
    total = parts.sum(axis=0)
    own = lax.all_to_all(jnp.broadcast_to(total[None], (8, 8, COLS)), ZX, 0, 0, tiled=True)
    own = own.reshape(HALF, COLS)
    partner = lax.ppermute(own, "co", flip(2, 1))
    near = lax.ppermute(own, ring, outer)
    half = solve(where, own, partner, near, visc, fric, drive, edge)
    rest = lax.ppermute(half, "co", flip(2, 1))
    first = core == 0
    ice_velocity = jnp.concatenate(
        [jnp.where(first, half, rest), jnp.where(first, rest, half)], axis=0
    )

    close, far = drafts(where, packets, thick)
    close = close + lax.ppermute(far, "xh", flip(2, 1))
    back = [lax.ppermute(close[k], "y", flip(4, k))[None] for k in range(1, 4)]
    temp_new = ocean(
        temp, uvel, vvel, below, above, west, east, col, cav, packet,
        close[0:1], *back, jnp.zeros_like(back[0]),
    )
    return temp_new, ice_velocity


def solution(mesh):
    finer = Mesh(mesh.devices.reshape(4, 2, 2, 2, 4), ("z", "xl", "co", "xh", "y"))
    field = P(None, GRP, BLK)
    entry = P(GRP, BLK, None)
    rows = P(BLK, None)
    return jax.shard_map(
        shards,
        mesh=finer,
        in_specs=(field,) * 3 + (entry,) * 3 + (rows,) * 4,
        out_specs=(field, rows),
        check_vma=False,
    )
```

```python
import functools
import jax
import jax.numpy as jnp
from jax import lax
from jax.experimental import pallas as pl
from jax.experimental.pallas import tpu as pltpu
from jax.sharding import Mesh
from jax.sharding import PartitionSpec as P


LEVELS = 3
CYCLES = 2
GRP = ("z", "xl", "co")
ZX = ("z", "xl")
BLK = ("xh", "y")
omega = 0.8
kappa = 0.1
vertical_mix = 0.2
melt_rate = 0.5

LEV = 8
CX = 64
CY = 128
ROWS = 128
COLS = 1024
HALF = 64
ENT = 2048
EXT = 192
KC = 512
CELLS = ROWS * COLS
f32 = jnp.float32
bf16 = jnp.bfloat16
i32 = jnp.int32
VMEM = pl.BlockSpec(memory_space=pltpu.VMEM)
SMEM = pl.BlockSpec(memory_space=pltpu.SMEM)


def cost(us):
    return pl.CostEstimate(flops=int(us * 2e7), bytes_accessed=0, transcendentals=0)


def split2(x):
    high = x.astype(bf16)
    low = (x - high.astype(f32)).astype(bf16)
    return high, low


def split3(x):
    high = x.astype(bf16)
    rest = x - high.astype(f32)
    mid = rest.astype(bf16)
    return high, mid, (rest - mid.astype(f32)).astype(bf16)


def sub_iota(shape):
    return lax.broadcasted_iota(i32, shape, 0)


def lane_iota(shape):
    return lax.broadcasted_iota(i32, shape, 1)


NT = (((1,), (1,)), ((), ()))


def pack_kernel(where, temp, uvel, vvel, col, cell, cav, packet, row_a, row_b, col_a, col_b):
    even_row, even_col = where[1] == 0, where[3] == 0
    tops = split3(temp[0].T)
    table = jnp.concatenate(tops, axis=0)
    for j in range(ENT // KC):
        c = col[0, :, j * KC : (j + 1) * KC]
        rows = jnp.where(sub_iota((CX, KC)) == (c >> 7), 1.0, 0.0).astype(bf16)
        picked = jnp.dot(table, rows, preferred_element_type=f32)
        picked = picked[0:128] + picked[128:256] + picked[256:384]
        mask = sub_iota((CY, KC)) == (c & 127)
        top = jnp.sum(jnp.where(mask, picked, 0.0), axis=0, keepdims=True)
        on = cav[0, :, j * KC : (j + 1) * KC] > 0
        index = jnp.where(on, cell[0, :, j * KC : (j + 1) * KC], -1)
        packet[0:1, j * KC : (j + 1) * KC] = index.astype(f32)
        packet[1:2, j * KC : (j + 1) * KC] = top
    for k in range(LEV):
        for field, at in ((temp, k), (uvel, k + 8)):
            low, high = field[k, 0:1, :], field[k, CX - 1 : CX, :]
            row_a[at : at + 1, :] = jnp.where(even_row, high, low)
            row_b[at : at + 1, :] = jnp.where(even_row, low, high)
        for field, at in ((temp, k), (vvel, k + 8)):
            across = field[k].T
            low, high = across[0:1, :], across[CY - 1 : CY, :]
            col_a[at : at + 1, :] = jnp.where(even_col, high, low)
            col_b[at : at + 1, :] = jnp.where(even_col, low, high)


def pack(where, temp, uvel, vvel, col, cell, cav):
    return pl.pallas_call(
        pack_kernel,
        out_shape=(
            jax.ShapeDtypeStruct((2, ENT), f32),
            jax.ShapeDtypeStruct((16, CY), f32),
            jax.ShapeDtypeStruct((16, CY), f32),
            jax.ShapeDtypeStruct((16, CX), f32),
            jax.ShapeDtypeStruct((16, CX), f32),
        ),
        in_specs=[SMEM] + [VMEM] * 6,
        out_specs=(VMEM,) * 5,
        cost_estimate=cost(3),
        name="pack",
    )(where, temp, uvel, vvel, col, cell, cav)


def place(packets, first, k):
    at = pl.multiple_of((k % (ENT // KC)) * KC, KC)
    index = packets[k // (ENT // KC), 0:1, pl.ds(at, KC)].astype(i32)
    local = index - first
    row = local >> 10
    spot = ((row >> 3) << 6) | (((local >> 7) & 7) << 3) | (row & 7)
    spot = jnp.where((local >= 0) & (local < CELLS), spot, -1)
    return spot, local & 127, at


def couple_kernel(where, packets, thick, mine, other, near, far, tiles, table, onehot, lanes, acc, melt):
    first, core = where[0], where[1]
    acc[...] = jnp.zeros_like(acc)
    for t in range(128):
        i, c = t // 8, t % 8
        tiles[t * 8 : t * 8 + 8, :] = thick[i * 8 : i * 8 + 8, c * 128 : c * 128 + 128]
    for a in range(8):
        high, low = split2(tiles[a * 128 : a * 128 + 128, :].T)
        table[0:128, a * 128 : a * 128 + 128] = high
        table[128:256, a * 128 : a * 128 + 128] = low

    def fetch(k, p, out):
        spot, lane, at = place(packets, first, k)
        onehot[p] = jnp.where(lax.broadcasted_iota(jnp.int16, (1024, KC), 0) == spot.astype(jnp.int16), jnp.array(1.0, bf16), jnp.array(0.0, bf16))
        picked = jnp.dot(table[...], onehot[p], preferred_element_type=f32)
        picked = picked[0:128] + picked[128:256]
        mask = sub_iota((128, KC)) == lane
        draft = jnp.sum(jnp.where(mask, picked, 0.0), axis=0, keepdims=True)
        s = k // (ENT // KC)
        out[s % 4, 0:1, pl.ds(at, KC)] = draft
        value = melt_rate * (packets[s, 1:2, pl.ds(at, KC)] + 0.5 + 0.5 * draft)
        high, low = split2(value)
        mask = lax.broadcasted_iota(jnp.int16, (128, KC), 0) == lane.astype(jnp.int16)
        zero = jnp.array(0.0, bf16)
        lanes[p, 0:128, :] = jnp.where(mask, high, zero)
        lanes[p, 128:256, :] = jnp.where(mask, low, zero)

    def spread(p):
        acc[...] += lax.dot_general(lanes[p], onehot[p], NT, preferred_element_type=f32)

    per = 4 * ENT // KC

    def near_chunk(h, carry):
        fetch(2 * h, 0, near)
        spread(1)
        fetch(2 * h + 1, 1, near)
        spread(0)
        return carry

    def far_chunk(h, carry):
        fetch(2 * h, 0, far)
        spread(1)
        fetch(2 * h + 1, 1, far)
        spread(0)
        return carry

    lanes[1] = jnp.zeros((256, KC), bf16)
    onehot[1] = jnp.zeros((1024, KC), bf16)
    lax.fori_loop(0, per // 2, near_chunk, 0)
    lax.fori_loop(per // 2, per, far_chunk, 0)
    spread(1)

    for a in range(8):
        at = slice(a * 128, a * 128 + 128)
        tiles[at, :] = (acc[0:128, at] + acc[128:256, at]).T
    for t in range(128):
        i, c = t // 8, t % 8
        melt[i // 8, (i % 8) * 8 : (i % 8) * 8 + 8, c * 128 : c * 128 + 128] = tiles[t * 8 : t * 8 + 8, :]
    mine[...] = melt[core]
    other[...] = melt[1 - core]


def couple(where, packets, thick):
    half = jax.ShapeDtypeStruct((HALF, COLS), f32)
    entry = jax.ShapeDtypeStruct((4, 1, ENT), f32)
    return pl.pallas_call(
        couple_kernel,
        out_shape=(half, half, entry, entry),
        in_specs=[SMEM, VMEM, VMEM],
        out_specs=(VMEM,) * 4,
        scratch_shapes=[
            pltpu.VMEM((1024, 128), f32),
            pltpu.VMEM((256, 1024), bf16),
            pltpu.VMEM((2, 1024, KC), bf16),
            pltpu.VMEM((2, 256, KC), bf16),
            pltpu.VMEM((256, 1024), f32),
            pltpu.VMEM((2, HALF, COLS), f32),
        ],
        cost_estimate=cost(24),
        name="couple",
    )(where, packets, thick)


def ocean_kernel(
    where, temp, uvel, vvel, row_a, row_b, col_a, col_b, col, cav, packet, d0, d1, d2, d3, out
):
    shape = (CX, CY)
    row, lane = sub_iota(shape), lane_iota(shape)
    heat = jnp.zeros((CX, 384), f32)
    for j in range(ENT // KC):
        at = slice(j * KC, (j + 1) * KC)
        draft = d0[0, :, at] + d1[0, :, at] + d2[0, :, at] + d3[0, :, at]
        c = col[0, :, at]
        melt = cav[0, :, at].astype(f32) * melt_rate * (packet[1:2, at] + 0.5 + 0.5 * draft)
        rows = jnp.where(sub_iota((CX, KC)) == (c >> 7), 1.0, 0.0).astype(bf16)
        mask = sub_iota((CY, KC)) == (c & 127)
        parts = [
            jnp.where(mask, part.astype(f32), 0.0).astype(bf16) for part in split3(melt)
        ]
        weights = jnp.concatenate(parts, axis=0)
        heat += lax.dot_general(rows, weights, NT, preferred_element_type=f32)
    column_melt = heat[:, 0:128] + heat[:, 128:256] + heat[:, 256:384]
    even_row, even_col = where[1] == 0, where[3] == 0
    above = jnp.where(even_row, row_a[...], row_b[...])
    below = jnp.where(even_row, row_b[...], row_a[...])
    first_t, second_t = col_a[...].T, col_b[...].T
    east_t = jnp.where(even_col, first_t, second_t)
    west_t = jnp.where(even_col, second_t, first_t)

    def nearby(field, k, side):
        x = field[k]
        e = jnp.where(row == CX - 1, above[side + k : side + k + 1, :], pltpu.roll(x, CX - 1, 0))
        w = jnp.where(row == 0, below[side + k : side + k + 1, :], pltpu.roll(x, 1, 0))
        return x, e, w

    def beside(field, k, side):
        x = field[k]
        n = jnp.where(lane == CY - 1, east_t[:, side + k : side + k + 1], pltpu.roll(x, CY - 1, 1))
        s = jnp.where(lane == 0, west_t[:, side + k : side + k + 1], pltpu.roll(x, 1, 1))
        return x, n, s

    for k in range(LEV):
        t, te, tw = nearby(temp, k, 0)
        _, tn, ts = beside(temp, k, 0)
        u, ue, uw = nearby(uvel, k, 8)
        v, vn, vs = beside(vvel, k, 8)
        speed = 0.5 * (u + ue)
        flux_east = jnp.maximum(speed, 0.0) * t + jnp.minimum(speed, 0.0) * te
        speed = 0.5 * (u + uw)
        flux_west = jnp.maximum(speed, 0.0) * tw + jnp.minimum(speed, 0.0) * t
        speed = 0.5 * (v + vn)
        flux_north = jnp.maximum(speed, 0.0) * t + jnp.minimum(speed, 0.0) * tn
        speed = 0.5 * (v + vs)
        flux_south = jnp.maximum(speed, 0.0) * ts + jnp.minimum(speed, 0.0) * t
        laplace = te + tw + tn + ts - 4.0 * t
        lower = temp[k + 1] - t if k + 1 < LEV else 0.0
        upper = t - temp[k - 1] if k else 0.0
        new = t + flux_west - flux_east + flux_south - flux_north
        new = new + kappa * laplace + vertical_mix * (lower - upper)
        out[k] = new - melt_rate * column_melt if k == 0 else new


def ocean(*arrays):
    return pl.pallas_call(
        ocean_kernel,
        out_shape=jax.ShapeDtypeStruct((LEV, CX, CY), f32),
        in_specs=[SMEM] + [VMEM] * (len(arrays) - 1),
        out_specs=VMEM,
        cost_estimate=cost(3),
        name="ocean",
    )(*arrays)


UP, DOWN, LEFT, RIGHT, INV, SCALE, G = range(7)


def solve_kernel(where, own, partner, near, visc, fric, drive, edge, out, *scratch):
    (vx, fx, sx, k0, k1, k2, v0, v1, v2, f1, f2, g2, res0, res1) = scratch
    core, base = where[1], where[2]
    zero8 = jnp.zeros((8, COLS), f32)

    def put(ref, rows, value):
        if len(ref.shape) == 2:
            ref[rows, :] = value
        else:
            for c in range(8):
                ref[c, rows, :] = value[:, c * 128 : c * 128 + 128]

    def take(ref, rows):
        if len(ref.shape) == 2:
            return ref[rows, :]
        return jnp.concatenate([ref[c, rows, :] for c in range(8)], axis=1)

    for ref in (vx, fx, sx):
        put(ref, slice(0, 8), zero8)
        put(ref, slice(EXT + 8, EXT + 16), zero8)

    for n, (block, full) in enumerate(((visc, vx), (fric, fx), (drive, sx))):

        @pl.when(core == 0)
        def _(n=n, block=block, full=full):
            put(full, slice(8, 72), edge[n])
            put(full, slice(72, 200), block[...])

        @pl.when(core == 1)
        def _(n=n, block=block, full=full):
            put(full, slice(8, 136), block[...])
            put(full, slice(136, 200), edge[n])

    sx[72:136, :] += own[...]

    @pl.when(core == 0)
    def _():
        sx[8:72, :] += near[...]
        sx[136:200, :] += partner[...]

    @pl.when(core == 1)
    def _():
        sx[8:72, :] += partner[...]
        sx[136:200, :] += near[...]

    lane = lane_iota((8, COLS))
    rowi = sub_iota((8, COLS))
    tiles = [EXT // 8 >> level for level in range(LEVELS)]
    ks = (k0, k1, k2)
    vs = (v0, v1, v2)

    def tile(i, d=1):
        if isinstance(i, int):
            return slice(8 * i + 8 * d, 8 * i + 8 * d + 8)
        return pl.ds(pl.multiple_of(8 * i + 8 * d, 8), 8)

    def shifted(ref, i):
        x = take(ref, tile(i))
        above = jnp.where(rowi == 7, take(ref, tile(i, 0)), x)
        below = jnp.where(rowi == 0, take(ref, tile(i, 2)), x)
        return pltpu.roll(above, 1, 0), pltpu.roll(below, 7, 0)

    def loop(lo, hi, body):
        for i in range(lo, hi):
            body(i)

    def left_of(x, s):
        return pltpu.roll(x, s, 1)

    def right_of(x, s):
        return pltpu.roll(x, COLS - s, 1)

    def halved(ref, i, s):
        def at(d):
            return take(ref, pl.ds(16 * i + 8 + d, 8, stride=2))

        pair = at(0) + at(1)
        beside = jnp.where((lane & s) == 0, right_of(pair, s), left_of(pair, s))
        return 0.25 * (pair + beside)

    viscs, frics = (vx, f1, f2), (fx, res1, g2)
    for level in range(LEVELS):
        s = 1 << level
        n = tiles[level]
        kr, vr, fr = ks[level], viscs[level], frics[level]
        if level:

            def coarsen(i, level=level, vr=vr, fr=fr, s=s):
                put(vr, tile(i), halved(viscs[level - 1], i, s // 2))
                put(fr, tile(i), halved(frics[level - 1], i, s // 2))

            put(vr, slice(0, 8), zero8)
            put(vr, slice(n * 8 + 8, n * 8 + 16), zero8)
            for i in range(n):
                coarsen(i)
        scale = 0.5 * 0.25**level
        start = base >> level

        def coefficients(i, level=level, kr=kr, vr=vr, fr=fr, s=s, scale=scale, start=start):
            x = take(vr, tile(i))
            above, below = shifted(vr, i)
            cu = scale * (x + above)
            cd = scale * (x + below)
            cl = scale * (x + jnp.where(lane < s, 0.0, left_of(x, s)))
            cr = scale * (x + jnp.where(lane >= COLS - s, 0.0, right_of(x, s)))
            diag = cu + cd + cl + cr + take(fr, tile(i))
            row = start + 8 * i + rowi
            inside = (row >= 0) & (row < (COLS >> level))
            inv = jnp.where(inside, omega / diag, 0.0)
            kr[UP, tile(i), :] = inv * cu
            kr[DOWN, tile(i), :] = inv * cd
            kr[LEFT, tile(i), :] = jnp.where(lane < s, 0.0, inv * cl)
            kr[RIGHT, tile(i), :] = jnp.where(lane >= COLS - s, 0.0, inv * cr)
            kr[SCALE, tile(i), :] = jnp.where(inside, diag * (1.0 / omega), 0.0)
            kr[INV, tile(i), :] = inv
            if level == 0:
                kr[G, tile(i), :] = inv * sx[tile(i), :]

        loop(0, n, coefficients)

    def step_of(level, src, i):
        kr, s = ks[level], 1 << level
        v = src[tile(i), :]
        above, below = shifted(src, i)
        total = kr[G, tile(i), :] + kr[UP, tile(i), :] * above + kr[DOWN, tile(i), :] * below
        total = total + kr[LEFT, tile(i), :] * left_of(v, s)
        total = total + kr[RIGHT, tile(i), :] * right_of(v, s)
        return v, total - omega * v

    def core_tiles(level, h):
        n = tiles[level]
        return max(n // 3 - h, 0), min(2 * n // 3 + h, n)

    def sweep(level, a, b, h):
        src, dst = vs[level].at[a], vs[level].at[b]

        def body(i):
            v, t = step_of(level, src, i)
            dst[tile(i), :] = v + t

        loop(*core_tiles(level, h), body)

    def residual(level, a, h, res):
        src = vs[level].at[a]

        def body(i):
            _, t = step_of(level, src, i)
            put(res, tile(i), t * ks[level][SCALE, tile(i), :])

        loop(*core_tiles(level, h), body)

    def free_sweep(level, a, h, source, s):
        kr, dst = ks[level], vs[level].at[a]

        def body(i):
            if source is not None:
                kr[G, tile(i), :] = kr[INV, tile(i), :] * halved(source, i, s)
            dst[tile(i), :] = kr[G, tile(i), :]

        if source is None:
            loop(*core_tiles(level, h), body)
            return
        for i in range(*core_tiles(level, h)):
            body(i)

    def correct(level, a, b, h, spread):
        fine, coarse = vs[level].at[a], vs[level + 1].at[b]
        lo, hi = core_tiles(level, h)

        def widen(i):
            e = coarse[tile(i), :]
            put(spread, pl.ds(16 * i + 8, 8, stride=2), e)
            put(spread, pl.ds(16 * i + 9, 8, stride=2), e)

        for i in range(lo // 2, (hi + 1) // 2):
            widen(i)

        def add(i):
            fine[tile(i), :] += take(spread, tile(i))

        loop(lo, hi, add)

    def clear(ref, i):
        put(ref, tile(i, 0), zero8)

    for level in range(LEVELS):
        for a in range(2):
            loop(0, tiles[level] + 2, functools.partial(clear, vs[level].at[a]))
    loop(0, tiles[0] + 2, functools.partial(clear, res0))
    loop(0, tiles[1] + 2, functools.partial(clear, res1))

    for cycle in range(CYCLES):
        first = cycle == 0
        now = 1
        if first:
            free_sweep(0, 0, 8, None, 1)
        else:
            sweep(0, 1, 0, 4)
        sweep(0, 0, 1, 8 if first else 4)
        residual(0, now, 7 if first else 4, res0)
        free_sweep(1, 0, 4 if first else 2, res0, 1)
        sweep(1, 0, 1, 4 if first else 2)
        residual(1, 1, 3 if first else 2, res1)
        h2 = 2 if first else 1
        free_sweep(2, 0, h2, res1, 2)
        sweep(2, 0, 1, h2)
        sweep(2, 1, 0, h2)
        sweep(2, 0, 1, h2)
        correct(1, 1, 1, 3 if first else 1, f1)
        sweep(1, 1, 0, 3 if first else 1)
        sweep(1, 0, 1, 3 if first else 1)
        correct(0, now, 1, 4 if first else 1, vx)
        sweep(0, now, 1 - now, 4 if first else 1)
        sweep(0, 1 - now, now, 4 if first else 0)
    out[...] = v0[1, 72:136, :]


def solve(where, own, partner, near, visc, fric, drive, edge):
    def rows(level, *lead):
        return pltpu.VMEM((*lead, (EXT >> level) + 16, COLS), f32)

    def blocks(level):
        return pltpu.VMEM((8, (EXT >> level) + 16, 128), f32)

    return pl.pallas_call(
        solve_kernel,
        out_shape=jax.ShapeDtypeStruct((HALF, COLS), f32),
        in_specs=[SMEM] + [VMEM] * 7,
        out_specs=VMEM,
        scratch_shapes=[
            blocks(0),
            blocks(0),
            rows(0),
            rows(0, 7),
            rows(1, 7),
            rows(2, 7),
            rows(0, 2),
            rows(1, 2),
            rows(2, 2),
            blocks(1),
            rows(2),
            rows(2),
            blocks(0),
            blocks(1),
        ],
        cost_estimate=cost(10),
        name="solve",
    )(where, own, partner, near, visc, fric, drive, edge)


def flip(n, k):
    return [(i, i ^ k) for i in range(n)]


def pairs(n, turn):
    later = [(i, i + 1) for i in range(turn, n - 1, 2)]
    return later + [(b, a) for a, b in later]


def step(temp, uvel, vvel, col, cell, cav, thick, visc, fric, drive):
    core = lax.axis_index("co").astype(i32)
    y = lax.axis_index("y").astype(i32)
    blk = lax.axis_index("xh").astype(i32) * 4 + y
    where = jnp.stack([blk * CELLS, core, blk * ROWS + core * HALF - 64, y & 1])

    packet, row_a, row_b, col_a, col_b = pack(where, temp, uvel, vvel, col, cell, cav)
    got = [packet] + [lax.ppermute(packet, "y", flip(4, k)) for k in range(1, 4)]
    got = jnp.stack(got)
    packets = jnp.concatenate([got, lax.ppermute(got, "xh", flip(2, 1))], axis=0)

    ring = ("co", "xh", "y")
    outer = [(b, 8 + b - 1) for b in range(1, 8)] + [(8 + b, b + 1) for b in range(7)]
    ice = jnp.stack([visc, fric, drive])
    ice_edge = lax.dynamic_slice_in_dim(ice, core * HALF, HALF, axis=1)
    edge = lax.ppermute(ice_edge, ring, outer)
    row_a = lax.ppermute(row_a, "co", flip(2, 1))
    row_b = lax.ppermute(row_b, GRP, pairs(16, 1))
    col_a = lax.ppermute(col_a, "y", flip(4, 1))
    col_b = lax.ppermute(col_b, BLK, pairs(8, 1))

    mine, other, close, far = couple(where, packets, thick)
    mine = mine + lax.ppermute(other, "co", flip(2, 1))
    far = lax.ppermute(far, "xh", flip(2, 1))
    parts = lax.all_to_all(mine.reshape(8, 8, COLS), ZX, 0, 0, tiled=True)
    total = parts.sum(axis=0)
    own = lax.all_to_all(jnp.broadcast_to(total[None], (8, 8, COLS)), ZX, 0, 0, tiled=True)
    own = own.reshape(HALF, COLS)
    partner = lax.ppermute(own, "co", flip(2, 1))
    near = lax.ppermute(own, ring, outer)
    close = close + far
    back = [lax.ppermute(close[k], "y", flip(4, k))[None] for k in range(1, 4)]
    half = solve(where, own, partner, near, visc, fric, drive, edge)
    rest = lax.ppermute(half, "co", flip(2, 1))
    temp_new = ocean(
        where, temp, uvel, vvel, row_a, row_b, col_a, col_b, col, cav, packet,
        close[0:1], *back,
    )
    first = core == 0
    ice_velocity = jnp.concatenate(
        [jnp.where(first, half, rest), jnp.where(first, rest, half)], axis=0
    )
    return temp_new, ice_velocity


def solution(mesh):
    finer = Mesh(mesh.devices.reshape(4, 2, 2, 2, 4), ("z", "xl", "co", "xh", "y"))
    field = P(None, GRP, BLK)
    entry = P(GRP, BLK, None)
    rows = P(BLK, None)
    return jax.shard_map(
        step,
        mesh=finer,
        in_specs=(field,) * 3 + (entry,) * 3 + (rows,) * 4,
        out_specs=(field, rows),
        check_vma=False,
    )
```

```python
import functools
import jax
import jax.numpy as jnp
from jax import lax
from jax.experimental import pallas as pl
from jax.experimental.pallas import tpu as pltpu
from jax.sharding import Mesh
from jax.sharding import PartitionSpec as P


LEVELS = 3
CYCLES = 2
GRP = ("z", "xl", "co")
BLK = ("xh", "y")
omega = 0.8
kappa = 0.1
vertical_mix = 0.2
melt_rate = 0.5

LEV = 8
CX = 64
CY = 128
ROWS = 128
COLS = 1024
HALF = 64
ENT = 2048
EXT = 192
KC = 512
CELLS = ROWS * COLS
f32 = jnp.float32
bf16 = jnp.bfloat16
i32 = jnp.int32
VMEM = pl.BlockSpec(memory_space=pltpu.VMEM)
SMEM = pl.BlockSpec(memory_space=pltpu.SMEM)


def cost(us):
    return pl.CostEstimate(flops=int(us * 2e7), bytes_accessed=0, transcendentals=0)


def split2(x):
    high = x.astype(bf16)
    low = (x - high.astype(f32)).astype(bf16)
    return high, low


def split3(x):
    high = x.astype(bf16)
    rest = x - high.astype(f32)
    mid = rest.astype(bf16)
    return high, mid, (rest - mid.astype(f32)).astype(bf16)


def sub_iota(shape):
    return lax.broadcasted_iota(i32, shape, 0)


def lane_iota(shape):
    return lax.broadcasted_iota(i32, shape, 1)


NT = (((1,), (1,)), ((), ()))


def pack_kernel(where, temp, uvel, vvel, col, cell, cav, packet, row_a, row_b, col_a, col_b):
    even_row, even_col = where[1] == 0, where[3] == 0
    tops = split3(temp[0].T)
    table = jnp.concatenate(tops, axis=0)
    for j in range(ENT // KC):
        c = col[0, :, j * KC : (j + 1) * KC]
        rows = jnp.where(sub_iota((CX, KC)) == (c >> 7), 1.0, 0.0).astype(bf16)
        picked = jnp.dot(table, rows, preferred_element_type=f32)
        picked = picked[0:128] + picked[128:256] + picked[256:384]
        mask = sub_iota((CY, KC)) == (c & 127)
        top = jnp.sum(jnp.where(mask, picked, 0.0), axis=0, keepdims=True)
        on = cav[0, :, j * KC : (j + 1) * KC] > 0
        index = jnp.where(on, cell[0, :, j * KC : (j + 1) * KC], -1)
        packet[0:1, j * KC : (j + 1) * KC] = index.astype(f32)
        packet[1:2, j * KC : (j + 1) * KC] = top
    for k in range(LEV):
        for field, at in ((temp, k), (uvel, k + 8)):
            low, high = field[k, 0:1, :], field[k, CX - 1 : CX, :]
            row_a[at : at + 1, :] = jnp.where(even_row, high, low)
            row_b[at : at + 1, :] = jnp.where(even_row, low, high)
        for field, at in ((temp, k), (vvel, k + 8)):
            across = field[k].T
            low, high = across[0:1, :], across[CY - 1 : CY, :]
            col_a[at : at + 1, :] = jnp.where(even_col, high, low)
            col_b[at : at + 1, :] = jnp.where(even_col, low, high)


def pack(where, temp, uvel, vvel, col, cell, cav):
    return pl.pallas_call(
        pack_kernel,
        out_shape=(
            jax.ShapeDtypeStruct((2, ENT), f32),
            jax.ShapeDtypeStruct((16, CY), f32),
            jax.ShapeDtypeStruct((16, CY), f32),
            jax.ShapeDtypeStruct((16, CX), f32),
            jax.ShapeDtypeStruct((16, CX), f32),
        ),
        in_specs=[SMEM] + [VMEM] * 6,
        out_specs=(VMEM,) * 5,
        cost_estimate=cost(3),
        name="pack",
    )(where, temp, uvel, vvel, col, cell, cav)


def place(packets, first, k):
    at = pl.multiple_of((k % (ENT // KC)) * KC, KC)
    index = packets[k // (ENT // KC), 0:1, pl.ds(at, KC)].astype(i32)
    local = index - first
    row = local >> 10
    spot = ((row >> 3) << 6) | (((local >> 7) & 7) << 3) | (row & 7)
    spot = jnp.where((local >= 0) & (local < CELLS), spot, -1)
    return spot, local & 127, at


def couple_kernel(where, packets, thick, mine, other, near, far, tiles, table, onehot, lanes, acc, melt):
    first, core = where[0], where[1]
    acc[...] = jnp.zeros_like(acc)
    for t in range(128):
        i, c = t // 8, t % 8
        tiles[t * 8 : t * 8 + 8, :] = thick[i * 8 : i * 8 + 8, c * 128 : c * 128 + 128]
    for a in range(8):
        high, low = split2(tiles[a * 128 : a * 128 + 128, :].T)
        table[0:128, a * 128 : a * 128 + 128] = high
        table[128:256, a * 128 : a * 128 + 128] = low

    def fetch(k, p, out):
        spot, lane, at = place(packets, first, k)
        onehot[p] = jnp.where(lax.broadcasted_iota(jnp.int16, (1024, KC), 0) == spot.astype(jnp.int16), jnp.array(1.0, bf16), jnp.array(0.0, bf16))
        picked = jnp.dot(table[...], onehot[p], preferred_element_type=f32)
        picked = picked[0:128] + picked[128:256]
        mask = sub_iota((128, KC)) == lane
        draft = jnp.sum(jnp.where(mask, picked, 0.0), axis=0, keepdims=True)
        s = k // (ENT // KC)
        out[s % 4, 0:1, pl.ds(at, KC)] = draft
        value = melt_rate * (packets[s, 1:2, pl.ds(at, KC)] + 0.5 + 0.5 * draft)
        high, low = split2(value)
        mask = lax.broadcasted_iota(jnp.int16, (128, KC), 0) == lane.astype(jnp.int16)
        zero = jnp.array(0.0, bf16)
        lanes[p, 0:128, :] = jnp.where(mask, high, zero)
        lanes[p, 128:256, :] = jnp.where(mask, low, zero)

    def spread(p):
        acc[...] += lax.dot_general(lanes[p], onehot[p], NT, preferred_element_type=f32)

    per = 4 * ENT // KC

    def near_chunk(h, carry):
        fetch(2 * h, 0, near)
        spread(1)
        fetch(2 * h + 1, 1, near)
        spread(0)
        return carry

    def far_chunk(h, carry):
        fetch(2 * h, 0, far)
        spread(1)
        fetch(2 * h + 1, 1, far)
        spread(0)
        return carry

    lanes[1] = jnp.zeros((256, KC), bf16)
    onehot[1] = jnp.zeros((1024, KC), bf16)
    lax.fori_loop(0, per // 2, near_chunk, 0)
    lax.fori_loop(per // 2, per, far_chunk, 0)
    spread(1)

    for a in range(8):
        at = slice(a * 128, a * 128 + 128)
        tiles[at, :] = (acc[0:128, at] + acc[128:256, at]).T
    for t in range(128):
        i, c = t // 8, t % 8
        melt[i // 8, (i % 8) * 8 : (i % 8) * 8 + 8, c * 128 : c * 128 + 128] = tiles[t * 8 : t * 8 + 8, :]
    mine[...] = melt[core]
    other[...] = melt[1 - core]


def couple(where, packets, thick):
    half = jax.ShapeDtypeStruct((HALF, COLS), f32)
    entry = jax.ShapeDtypeStruct((4, 1, ENT), f32)
    return pl.pallas_call(
        couple_kernel,
        out_shape=(half, half, entry, entry),
        in_specs=[SMEM, VMEM, VMEM],
        out_specs=(VMEM,) * 4,
        scratch_shapes=[
            pltpu.VMEM((1024, 128), f32),
            pltpu.VMEM((256, 1024), bf16),
            pltpu.VMEM((2, 1024, KC), bf16),
            pltpu.VMEM((2, 256, KC), bf16),
            pltpu.VMEM((256, 1024), f32),
            pltpu.VMEM((2, HALF, COLS), f32),
        ],
        cost_estimate=cost(24),
        name="couple",
    )(where, packets, thick)


def ocean_kernel(
    where, temp, uvel, vvel, row_a, row_b, col_a, col_b, col, cav, packet, d0, d1, d2, d3, out
):
    shape = (CX, CY)
    row, lane = sub_iota(shape), lane_iota(shape)
    heat = jnp.zeros((CX, 384), f32)
    for j in range(ENT // KC):
        at = slice(j * KC, (j + 1) * KC)
        draft = d0[0, :, at] + d1[0, :, at] + d2[0, :, at] + d3[0, :, at]
        c = col[0, :, at]
        melt = cav[0, :, at].astype(f32) * melt_rate * (packet[1:2, at] + 0.5 + 0.5 * draft)
        rows = jnp.where(sub_iota((CX, KC)) == (c >> 7), 1.0, 0.0).astype(bf16)
        mask = sub_iota((CY, KC)) == (c & 127)
        parts = [
            jnp.where(mask, part.astype(f32), 0.0).astype(bf16) for part in split3(melt)
        ]
        weights = jnp.concatenate(parts, axis=0)
        heat += lax.dot_general(rows, weights, NT, preferred_element_type=f32)
    column_melt = heat[:, 0:128] + heat[:, 128:256] + heat[:, 256:384]
    even_row, even_col = where[1] == 0, where[3] == 0
    above = jnp.where(even_row, row_a[...], row_b[...])
    below = jnp.where(even_row, row_b[...], row_a[...])
    first_t, second_t = col_a[...].T, col_b[...].T
    east_t = jnp.where(even_col, first_t, second_t)
    west_t = jnp.where(even_col, second_t, first_t)

    def nearby(field, k, side):
        x = field[k]
        e = jnp.where(row == CX - 1, above[side + k : side + k + 1, :], pltpu.roll(x, CX - 1, 0))
        w = jnp.where(row == 0, below[side + k : side + k + 1, :], pltpu.roll(x, 1, 0))
        return x, e, w

    def beside(field, k, side):
        x = field[k]
        n = jnp.where(lane == CY - 1, east_t[:, side + k : side + k + 1], pltpu.roll(x, CY - 1, 1))
        s = jnp.where(lane == 0, west_t[:, side + k : side + k + 1], pltpu.roll(x, 1, 1))
        return x, n, s

    for k in range(LEV):
        t, te, tw = nearby(temp, k, 0)
        _, tn, ts = beside(temp, k, 0)
        u, ue, uw = nearby(uvel, k, 8)
        v, vn, vs = beside(vvel, k, 8)
        speed = 0.5 * (u + ue)
        flux_east = jnp.maximum(speed, 0.0) * t + jnp.minimum(speed, 0.0) * te
        speed = 0.5 * (u + uw)
        flux_west = jnp.maximum(speed, 0.0) * tw + jnp.minimum(speed, 0.0) * t
        speed = 0.5 * (v + vn)
        flux_north = jnp.maximum(speed, 0.0) * t + jnp.minimum(speed, 0.0) * tn
        speed = 0.5 * (v + vs)
        flux_south = jnp.maximum(speed, 0.0) * ts + jnp.minimum(speed, 0.0) * t
        laplace = te + tw + tn + ts - 4.0 * t
        lower = temp[k + 1] - t if k + 1 < LEV else 0.0
        upper = t - temp[k - 1] if k else 0.0
        new = t + flux_west - flux_east + flux_south - flux_north
        new = new + kappa * laplace + vertical_mix * (lower - upper)
        out[k] = new - melt_rate * column_melt if k == 0 else new


def ocean(*arrays):
    return pl.pallas_call(
        ocean_kernel,
        out_shape=jax.ShapeDtypeStruct((LEV, CX, CY), f32),
        in_specs=[SMEM] + [VMEM] * (len(arrays) - 1),
        out_specs=VMEM,
        cost_estimate=cost(3),
        name="ocean",
    )(*arrays)


UP, DOWN, LEFT, RIGHT, INV, SCALE, G = range(7)


def solve_kernel(where, own, partner, near, visc, fric, drive, edge, out, *scratch):
    (vx, fx, sx, k0, k1, k2, v0, v1, v2, f1, f2, g2, res0, res1) = scratch
    core, base = where[1], where[2]
    zero8 = jnp.zeros((8, COLS), f32)

    def put(ref, rows, value):
        if len(ref.shape) == 2:
            ref[rows, :] = value
        else:
            for c in range(8):
                ref[c, rows, :] = value[:, c * 128 : c * 128 + 128]

    def take(ref, rows):
        if len(ref.shape) == 2:
            return ref[rows, :]
        return jnp.concatenate([ref[c, rows, :] for c in range(8)], axis=1)

    for ref in (vx, fx, sx):
        put(ref, slice(0, 8), zero8)
        put(ref, slice(EXT + 8, EXT + 16), zero8)

    for n, (block, full) in enumerate(((visc, vx), (fric, fx), (drive, sx))):

        @pl.when(core == 0)
        def _(n=n, block=block, full=full):
            put(full, slice(8, 72), edge[n])
            put(full, slice(72, 200), block[...])

        @pl.when(core == 1)
        def _(n=n, block=block, full=full):
            put(full, slice(8, 136), block[...])
            put(full, slice(136, 200), edge[n])

    sx[72:136, :] += own[...]

    @pl.when(core == 0)
    def _():
        sx[8:72, :] += near[...]
        sx[136:200, :] += partner[...]

    @pl.when(core == 1)
    def _():
        sx[8:72, :] += partner[...]
        sx[136:200, :] += near[...]

    lane = lane_iota((8, COLS))
    rowi = sub_iota((8, COLS))
    tiles = [EXT // 8 >> level for level in range(LEVELS)]
    ks = (k0, k1, k2)
    vs = (v0, v1, v2)

    def tile(i, d=1):
        if isinstance(i, int):
            return slice(8 * i + 8 * d, 8 * i + 8 * d + 8)
        return pl.ds(pl.multiple_of(8 * i + 8 * d, 8), 8)

    def shifted(ref, i):
        x = take(ref, tile(i))
        above = jnp.where(rowi == 7, take(ref, tile(i, 0)), x)
        below = jnp.where(rowi == 0, take(ref, tile(i, 2)), x)
        return pltpu.roll(above, 1, 0), pltpu.roll(below, 7, 0)

    def loop(lo, hi, body):
        for i in range(lo, hi):
            body(i)

    def left_of(x, s):
        return pltpu.roll(x, s, 1)

    def right_of(x, s):
        return pltpu.roll(x, COLS - s, 1)

    def halved(ref, i, s):
        def at(d):
            return take(ref, pl.ds(16 * i + 8 + d, 8, stride=2))

        pair = at(0) + at(1)
        beside = jnp.where((lane & s) == 0, right_of(pair, s), left_of(pair, s))
        return 0.25 * (pair + beside)

    viscs, frics = (vx, f1, f2), (fx, res1, g2)
    for level in range(LEVELS):
        s = 1 << level
        n = tiles[level]
        kr, vr, fr = ks[level], viscs[level], frics[level]
        if level:

            def coarsen(i, level=level, vr=vr, fr=fr, s=s):
                put(vr, tile(i), halved(viscs[level - 1], i, s // 2))
                put(fr, tile(i), halved(frics[level - 1], i, s // 2))

            put(vr, slice(0, 8), zero8)
            put(vr, slice(n * 8 + 8, n * 8 + 16), zero8)
            for i in range(n):
                coarsen(i)
        scale = 0.5 * 0.25**level
        start = base >> level

        def coefficients(i, level=level, kr=kr, vr=vr, fr=fr, s=s, scale=scale, start=start):
            x = take(vr, tile(i))
            above, below = shifted(vr, i)
            cu = scale * (x + above)
            cd = scale * (x + below)
            cl = scale * (x + jnp.where(lane < s, 0.0, left_of(x, s)))
            cr = scale * (x + jnp.where(lane >= COLS - s, 0.0, right_of(x, s)))
            diag = cu + cd + cl + cr + take(fr, tile(i))
            row = start + 8 * i + rowi
            inside = (row >= 0) & (row < (COLS >> level))
            inv = jnp.where(inside, omega / diag, 0.0)
            kr[UP, tile(i), :] = inv * cu
            kr[DOWN, tile(i), :] = inv * cd
            kr[LEFT, tile(i), :] = jnp.where(lane < s, 0.0, inv * cl)
            kr[RIGHT, tile(i), :] = jnp.where(lane >= COLS - s, 0.0, inv * cr)
            kr[SCALE, tile(i), :] = jnp.where(inside, diag * (1.0 / omega), 0.0)
            kr[INV, tile(i), :] = inv
            if level == 0:
                kr[G, tile(i), :] = inv * sx[tile(i), :]

        loop(0, n, coefficients)

    def step_of(level, src, i):
        kr, s = ks[level], 1 << level
        v = src[tile(i), :]
        above, below = shifted(src, i)
        total = kr[G, tile(i), :] + kr[UP, tile(i), :] * above + kr[DOWN, tile(i), :] * below
        total = total + kr[LEFT, tile(i), :] * left_of(v, s)
        total = total + kr[RIGHT, tile(i), :] * right_of(v, s)
        return v, total - omega * v

    def core_tiles(level, h):
        n = tiles[level]
        return max(n // 3 - h, 0), min(2 * n // 3 + h, n)

    def sweep(level, a, b, h):
        src, dst = vs[level].at[a], vs[level].at[b]

        def body(i):
            v, t = step_of(level, src, i)
            dst[tile(i), :] = v + t

        loop(*core_tiles(level, h), body)

    def residual(level, a, h, res):
        src = vs[level].at[a]

        def body(i):
            _, t = step_of(level, src, i)
            put(res, tile(i), t * ks[level][SCALE, tile(i), :])

        loop(*core_tiles(level, h), body)

    def free_sweep(level, a, h, source, s):
        kr, dst = ks[level], vs[level].at[a]

        def body(i):
            if source is not None:
                kr[G, tile(i), :] = kr[INV, tile(i), :] * halved(source, i, s)
            dst[tile(i), :] = kr[G, tile(i), :]

        if source is None:
            loop(*core_tiles(level, h), body)
            return
        for i in range(*core_tiles(level, h)):
            body(i)

    def correct(level, a, b, h, spread):
        fine, coarse = vs[level].at[a], vs[level + 1].at[b]
        lo, hi = core_tiles(level, h)

        def widen(i):
            e = coarse[tile(i), :]
            put(spread, pl.ds(16 * i + 8, 8, stride=2), e)
            put(spread, pl.ds(16 * i + 9, 8, stride=2), e)

        for i in range(lo // 2, (hi + 1) // 2):
            widen(i)

        def add(i):
            fine[tile(i), :] += take(spread, tile(i))

        loop(lo, hi, add)

    def clear(ref, i):
        put(ref, tile(i, 0), zero8)

    for level in range(LEVELS):
        for a in range(2):
            loop(0, tiles[level] + 2, functools.partial(clear, vs[level].at[a]))
    loop(0, tiles[0] + 2, functools.partial(clear, res0))
    loop(0, tiles[1] + 2, functools.partial(clear, res1))

    for cycle in range(CYCLES):
        first = cycle == 0
        now = 1
        if first:
            free_sweep(0, 0, 8, None, 1)
        else:
            sweep(0, 1, 0, 4)
        sweep(0, 0, 1, 8 if first else 4)
        residual(0, now, 7 if first else 4, res0)
        free_sweep(1, 0, 4 if first else 2, res0, 1)
        sweep(1, 0, 1, 4 if first else 2)
        residual(1, 1, 3 if first else 2, res1)
        h2 = 2 if first else 1
        free_sweep(2, 0, h2, res1, 2)
        sweep(2, 0, 1, h2)
        sweep(2, 1, 0, h2)
        sweep(2, 0, 1, h2)
        correct(1, 1, 1, 3 if first else 1, f1)
        sweep(1, 1, 0, 3 if first else 1)
        sweep(1, 0, 1, 3 if first else 1)
        correct(0, now, 1, 4 if first else 1, vx)
        sweep(0, now, 1 - now, 4 if first else 1)
        sweep(0, 1 - now, now, 4 if first else 0)
    out[...] = v0[1, 72:136, :]


def solve(where, own, partner, near, visc, fric, drive, edge):
    def rows(level, *lead):
        return pltpu.VMEM((*lead, (EXT >> level) + 16, COLS), f32)

    def blocks(level):
        return pltpu.VMEM((8, (EXT >> level) + 16, 128), f32)

    return pl.pallas_call(
        solve_kernel,
        out_shape=jax.ShapeDtypeStruct((HALF, COLS), f32),
        in_specs=[SMEM] + [VMEM] * 7,
        out_specs=VMEM,
        scratch_shapes=[
            blocks(0),
            blocks(0),
            rows(0),
            rows(0, 7),
            rows(1, 7),
            rows(2, 7),
            rows(0, 2),
            rows(1, 2),
            rows(2, 2),
            blocks(1),
            rows(2),
            rows(2),
            blocks(0),
            blocks(1),
        ],
        cost_estimate=cost(10),
        name="solve",
    )(where, own, partner, near, visc, fric, drive, edge)


def flip(n, k):
    return [(i, i ^ k) for i in range(n)]


def pairs(n, turn):
    later = [(i, i + 1) for i in range(turn, n - 1, 2)]
    return later + [(b, a) for a, b in later]


def step(temp, uvel, vvel, col, cell, cav, thick, visc, fric, drive):
    core = lax.axis_index("co").astype(i32)
    y = lax.axis_index("y").astype(i32)
    blk = lax.axis_index("xh").astype(i32) * 4 + y
    where = jnp.stack([blk * CELLS, core, blk * ROWS + core * HALF - 64, y & 1])

    packet, row_a, row_b, col_a, col_b = pack(where, temp, uvel, vvel, col, cell, cav)
    got = [packet] + [lax.ppermute(packet, "y", flip(4, k)) for k in range(1, 4)]
    got = jnp.stack(got)
    packets = jnp.concatenate([got, lax.ppermute(got, "xh", flip(2, 1))], axis=0)

    ring = ("co", "xh", "y")
    outer = [(b, 8 + b - 1) for b in range(1, 8)] + [(8 + b, b + 1) for b in range(7)]
    ice = jnp.stack([visc, fric, drive])
    ice_edge = lax.dynamic_slice_in_dim(ice, core * HALF, HALF, axis=1)
    edge = lax.ppermute(ice_edge, ring, outer)
    row_a = lax.ppermute(row_a, "co", flip(2, 1))
    row_b = lax.ppermute(row_b, GRP, pairs(16, 1))
    col_a = lax.ppermute(col_a, "y", flip(4, 1))
    col_b = lax.ppermute(col_b, BLK, pairs(8, 1))

    mine, other, close, far = couple(where, packets, thick)
    theirs = lax.ppermute(other, "co", flip(2, 1))
    far = lax.ppermute(far, "xh", flip(2, 1))
    part_a = mine[:32] + theirs[:32]
    part_b = mine[32:] + theirs[32:]
    ways = {"xl": flip(2, 1), "z": flip(4, 1)}
    around = [(i, 3 - i) for i in range(4)]
    part_a = part_a + lax.ppermute(part_a, "xl", ways["xl"])
    part_b = part_b + lax.ppermute(part_b, "z", ways["z"])
    part_a = part_a + lax.ppermute(part_a, "z", ways["z"])
    part_b = part_b + lax.ppermute(part_b, "z", around)
    close = close + far
    back = [lax.ppermute(close[k], "y", flip(4, k))[None] for k in range(1, 4)]
    part_a = part_a + lax.ppermute(part_a, "z", around)
    part_b = part_b + lax.ppermute(part_b, "xl", ways["xl"])
    own = jnp.concatenate([part_a, part_b], axis=0)
    partner = lax.ppermute(own, "co", flip(2, 1))
    near = lax.ppermute(own, ring, outer)
    half = solve(where, own, partner, near, visc, fric, drive, edge)
    rest = lax.ppermute(half, "co", flip(2, 1))
    temp_new = ocean(
        where, temp, uvel, vvel, row_a, row_b, col_a, col_b, col, cav, packet,
        close[0:1], *back,
    )
    first = core == 0
    ice_velocity = jnp.concatenate(
        [jnp.where(first, half, rest), jnp.where(first, rest, half)], axis=0
    )
    return temp_new, ice_velocity


def solution(mesh):
    finer = Mesh(mesh.devices.reshape(4, 2, 2, 2, 4), ("z", "xl", "co", "xh", "y"))
    field = P(None, GRP, BLK)
    entry = P(GRP, BLK, None)
    rows = P(BLK, None)
    return jax.shard_map(
        step,
        mesh=finer,
        in_specs=(field,) * 3 + (entry,) * 3 + (rows,) * 4,
        out_specs=(field, rows),
        check_vma=False,
    )
```

```python
import functools
import jax
import jax.numpy as jnp
from jax import lax
from jax.experimental import pallas as pl
from jax.experimental.pallas import tpu as pltpu
from jax.sharding import Mesh
from jax.sharding import PartitionSpec as P


LEVELS = 3
CYCLES = 2
GRP = ("z", "xl", "co")
BLK = ("xh", "y")
omega = 0.8
kappa = 0.1
vertical_mix = 0.2
melt_rate = 0.5

LEV = 8
CX = 64
CY = 128
ROWS = 128
COLS = 1024
HALF = 64
ENT = 2048
EXT = 192
KC = 1024
CELLS = ROWS * COLS
f32 = jnp.float32
bf16 = jnp.bfloat16
i32 = jnp.int32
VMEM = pl.BlockSpec(memory_space=pltpu.VMEM)
SMEM = pl.BlockSpec(memory_space=pltpu.SMEM)


def cost(us):
    return pl.CostEstimate(flops=int(us * 2e7), bytes_accessed=0, transcendentals=0)


def split2(x):
    high = x.astype(bf16)
    low = (x - high.astype(f32)).astype(bf16)
    return high, low


def split3(x):
    high = x.astype(bf16)
    rest = x - high.astype(f32)
    mid = rest.astype(bf16)
    return high, mid, (rest - mid.astype(f32)).astype(bf16)


def sub_iota(shape):
    return lax.broadcasted_iota(i32, shape, 0)


def lane_iota(shape):
    return lax.broadcasted_iota(i32, shape, 1)


NT = (((1,), (1,)), ((), ()))


def pack_kernel(where, temp, uvel, vvel, col, cell, cav, packet, row_a, row_b, col_a, col_b):
    even_row, even_col = where[1] == 0, where[3] == 0
    tops = split3(temp[0].T)
    table = jnp.concatenate(tops, axis=0)
    for j in range(ENT // KC):
        c = col[0, :, j * KC : (j + 1) * KC]
        rows = jnp.where(sub_iota((CX, KC)) == (c >> 7), 1.0, 0.0).astype(bf16)
        picked = jnp.dot(table, rows, preferred_element_type=f32)
        picked = picked[0:128] + picked[128:256] + picked[256:384]
        mask = sub_iota((CY, KC)) == (c & 127)
        top = jnp.sum(jnp.where(mask, picked, 0.0), axis=0, keepdims=True)
        on = cav[0, :, j * KC : (j + 1) * KC] > 0
        index = jnp.where(on, cell[0, :, j * KC : (j + 1) * KC], -1)
        packet[0:1, j * KC : (j + 1) * KC] = index.astype(f32)
        packet[1:2, j * KC : (j + 1) * KC] = top
    for k in range(LEV):
        for field, at in ((temp, k), (uvel, k + 8)):
            low, high = field[k, 0:1, :], field[k, CX - 1 : CX, :]
            row_a[at : at + 1, :] = jnp.where(even_row, high, low)
            row_b[at : at + 1, :] = jnp.where(even_row, low, high)
        for field, at in ((temp, k), (vvel, k + 8)):
            across = field[k].T
            low, high = across[0:1, :], across[CY - 1 : CY, :]
            col_a[at : at + 1, :] = jnp.where(even_col, high, low)
            col_b[at : at + 1, :] = jnp.where(even_col, low, high)


def pack(where, temp, uvel, vvel, col, cell, cav):
    return pl.pallas_call(
        pack_kernel,
        out_shape=(
            jax.ShapeDtypeStruct((2, ENT), f32),
            jax.ShapeDtypeStruct((16, CY), f32),
            jax.ShapeDtypeStruct((16, CY), f32),
            jax.ShapeDtypeStruct((16, CX), f32),
            jax.ShapeDtypeStruct((16, CX), f32),
        ),
        in_specs=[SMEM] + [VMEM] * 6,
        out_specs=(VMEM,) * 5,
        cost_estimate=cost(3),
        name="pack",
    )(where, temp, uvel, vvel, col, cell, cav)


def place(packets, first, k):
    at = pl.multiple_of((k % (ENT // KC)) * KC, KC)
    index = packets[k // (ENT // KC) % 4, 0:1, pl.ds(at, KC)].astype(i32)
    local = index - first
    row = local >> 10
    spot = ((row >> 3) << 6) | (((local >> 7) & 7) << 3) | (row & 7)
    spot = jnp.where((local >= 0) & (local < CELLS), spot, -1)
    return spot, local & 127, at


def couple_kernel(where, close, away, thick, mine, other, near, far, tiles, table, onehot, lanes, acc, melt):
    first, core = where[0], where[1]
    acc[...] = jnp.zeros_like(acc)
    for t in range(128):
        i, c = t // 8, t % 8
        tiles[t * 8 : t * 8 + 8, :] = thick[i * 8 : i * 8 + 8, c * 128 : c * 128 + 128]
    for a in range(8):
        high, low = split2(tiles[a * 128 : a * 128 + 128, :].T)
        table[0:128, a * 128 : a * 128 + 128] = high
        table[128:256, a * 128 : a * 128 + 128] = low

    def fetch(k, p, packets, out):
        spot, lane, at = place(packets, first, k)
        onehot[p] = jnp.where(lax.broadcasted_iota(jnp.int16, (1024, KC), 0) == spot.astype(jnp.int16), jnp.array(1.0, bf16), jnp.array(0.0, bf16))
        picked = jnp.dot(table[...], onehot[p], preferred_element_type=f32)
        picked = picked[0:128] + picked[128:256]
        mask = sub_iota((128, KC)) == lane
        draft = jnp.sum(jnp.where(mask, picked, 0.0), axis=0, keepdims=True)
        s = k // (ENT // KC)
        out[s % 4, 0:1, pl.ds(at, KC)] = draft
        value = melt_rate * (packets[s % 4, 1:2, pl.ds(at, KC)] + 0.5 + 0.5 * draft)
        high, low = split2(value)
        mask = lax.broadcasted_iota(jnp.int16, (128, KC), 0) == lane.astype(jnp.int16)
        zero = jnp.array(0.0, bf16)
        lanes[p, 0:128, :] = jnp.where(mask, high, zero)
        lanes[p, 128:256, :] = jnp.where(mask, low, zero)

    def spread(p):
        acc[...] += lax.dot_general(lanes[p], onehot[p], NT, preferred_element_type=f32)

    per = 4 * ENT // KC

    def near_chunk(h, carry):
        fetch(2 * h, 0, close, near)
        spread(1)
        fetch(2 * h + 1, 1, close, near)
        spread(0)
        return carry

    def far_chunk(h, carry):
        fetch(2 * h, 0, away, far)
        spread(1)
        fetch(2 * h + 1, 1, away, far)
        spread(0)
        return carry

    lanes[1] = jnp.zeros((256, KC), bf16)
    onehot[1] = jnp.zeros((1024, KC), bf16)
    lax.fori_loop(0, per // 2, near_chunk, 0)
    lax.fori_loop(per // 2, per, far_chunk, 0)
    spread(1)

    for a in range(8):
        at = slice(a * 128, a * 128 + 128)
        tiles[at, :] = (acc[0:128, at] + acc[128:256, at]).T
    for t in range(128):
        i, c = t // 8, t % 8
        melt[i // 8, (i % 8) * 8 : (i % 8) * 8 + 8, c * 128 : c * 128 + 128] = tiles[t * 8 : t * 8 + 8, :]
    mine[...] = melt[core]
    other[...] = melt[1 - core]


def couple(where, close, away, thick):
    half = jax.ShapeDtypeStruct((HALF, COLS), f32)
    entry = jax.ShapeDtypeStruct((4, 1, ENT), f32)
    return pl.pallas_call(
        couple_kernel,
        out_shape=(half, half, entry, entry),
        in_specs=[SMEM, VMEM, VMEM, VMEM],
        out_specs=(VMEM,) * 4,
        scratch_shapes=[
            pltpu.VMEM((1024, 128), f32),
            pltpu.VMEM((256, 1024), bf16),
            pltpu.VMEM((2, 1024, KC), bf16),
            pltpu.VMEM((2, 256, KC), bf16),
            pltpu.VMEM((256, 1024), f32),
            pltpu.VMEM((2, HALF, COLS), f32),
        ],
        cost_estimate=cost(24),
        name="couple",
    )(where, close, away, thick)


def ocean_kernel(
    where, temp, uvel, vvel, row_a, row_b, col_a, col_b, col, cav, packet, d0, d1, d2, d3, out
):
    shape = (CX, CY)
    row, lane = sub_iota(shape), lane_iota(shape)
    heat = jnp.zeros((CX, 384), f32)
    for j in range(ENT // KC):
        at = slice(j * KC, (j + 1) * KC)
        draft = d0[0, :, at] + d1[0, :, at] + d2[0, :, at] + d3[0, :, at]
        c = col[0, :, at]
        melt = cav[0, :, at].astype(f32) * melt_rate * (packet[1:2, at] + 0.5 + 0.5 * draft)
        rows = jnp.where(sub_iota((CX, KC)) == (c >> 7), 1.0, 0.0).astype(bf16)
        mask = sub_iota((CY, KC)) == (c & 127)
        parts = [
            jnp.where(mask, part.astype(f32), 0.0).astype(bf16) for part in split3(melt)
        ]
        weights = jnp.concatenate(parts, axis=0)
        heat += lax.dot_general(rows, weights, NT, preferred_element_type=f32)
    column_melt = heat[:, 0:128] + heat[:, 128:256] + heat[:, 256:384]
    even_row, even_col = where[1] == 0, where[3] == 0
    above = jnp.where(even_row, row_a[...], row_b[...])
    below = jnp.where(even_row, row_b[...], row_a[...])
    first_t, second_t = col_a[...].T, col_b[...].T
    east_t = jnp.where(even_col, first_t, second_t)
    west_t = jnp.where(even_col, second_t, first_t)

    def nearby(field, k, side):
        x = field[k]
        e = jnp.where(row == CX - 1, above[side + k : side + k + 1, :], pltpu.roll(x, CX - 1, 0))
        w = jnp.where(row == 0, below[side + k : side + k + 1, :], pltpu.roll(x, 1, 0))
        return x, e, w

    def beside(field, k, side):
        x = field[k]
        n = jnp.where(lane == CY - 1, east_t[:, side + k : side + k + 1], pltpu.roll(x, CY - 1, 1))
        s = jnp.where(lane == 0, west_t[:, side + k : side + k + 1], pltpu.roll(x, 1, 1))
        return x, n, s

    for k in range(LEV):
        t, te, tw = nearby(temp, k, 0)
        _, tn, ts = beside(temp, k, 0)
        u, ue, uw = nearby(uvel, k, 8)
        v, vn, vs = beside(vvel, k, 8)
        speed = 0.5 * (u + ue)
        flux_east = jnp.maximum(speed, 0.0) * t + jnp.minimum(speed, 0.0) * te
        speed = 0.5 * (u + uw)
        flux_west = jnp.maximum(speed, 0.0) * tw + jnp.minimum(speed, 0.0) * t
        speed = 0.5 * (v + vn)
        flux_north = jnp.maximum(speed, 0.0) * t + jnp.minimum(speed, 0.0) * tn
        speed = 0.5 * (v + vs)
        flux_south = jnp.maximum(speed, 0.0) * ts + jnp.minimum(speed, 0.0) * t
        laplace = te + tw + tn + ts - 4.0 * t
        lower = temp[k + 1] - t if k + 1 < LEV else 0.0
        upper = t - temp[k - 1] if k else 0.0
        new = t + flux_west - flux_east + flux_south - flux_north
        new = new + kappa * laplace + vertical_mix * (lower - upper)
        out[k] = new - melt_rate * column_melt if k == 0 else new


def ocean(*arrays):
    return pl.pallas_call(
        ocean_kernel,
        out_shape=jax.ShapeDtypeStruct((LEV, CX, CY), f32),
        in_specs=[SMEM] + [VMEM] * (len(arrays) - 1),
        out_specs=VMEM,
        cost_estimate=cost(3),
        name="ocean",
    )(*arrays)


UP, DOWN, LEFT, RIGHT, INV, SCALE, G = range(7)


def solve_kernel(where, own, partner, near, visc, fric, drive, edge, out, *scratch):
    (vx, fx, sx, k0, k1, k2, v0, v1, v2, f1, f2, g2, res0, res1) = scratch
    core, base = where[1], where[2]
    zero8 = jnp.zeros((8, COLS), f32)

    def put(ref, rows, value):
        if len(ref.shape) == 2:
            ref[rows, :] = value
        else:
            for c in range(8):
                ref[c, rows, :] = value[:, c * 128 : c * 128 + 128]

    def take(ref, rows):
        if len(ref.shape) == 2:
            return ref[rows, :]
        return jnp.concatenate([ref[c, rows, :] for c in range(8)], axis=1)

    for ref in (vx, fx, sx):
        put(ref, slice(0, 8), zero8)
        put(ref, slice(EXT + 8, EXT + 16), zero8)

    for n, (block, full) in enumerate(((visc, vx), (fric, fx), (drive, sx))):

        @pl.when(core == 0)
        def _(n=n, block=block, full=full):
            put(full, slice(8, 72), edge[n])
            put(full, slice(72, 200), block[...])

        @pl.when(core == 1)
        def _(n=n, block=block, full=full):
            put(full, slice(8, 136), block[...])
            put(full, slice(136, 200), edge[n])

    sx[72:136, :] += own[...]

    @pl.when(core == 0)
    def _():
        sx[8:72, :] += near[...]
        sx[136:200, :] += partner[...]

    @pl.when(core == 1)
    def _():
        sx[8:72, :] += partner[...]
        sx[136:200, :] += near[...]

    lane = lane_iota((8, COLS))
    rowi = sub_iota((8, COLS))
    tiles = [EXT // 8 >> level for level in range(LEVELS)]
    ks = (k0, k1, k2)
    vs = (v0, v1, v2)

    def tile(i, d=1):
        if isinstance(i, int):
            return slice(8 * i + 8 * d, 8 * i + 8 * d + 8)
        return pl.ds(pl.multiple_of(8 * i + 8 * d, 8), 8)

    def shifted(ref, i):
        x = take(ref, tile(i))
        above = jnp.where(rowi == 7, take(ref, tile(i, 0)), x)
        below = jnp.where(rowi == 0, take(ref, tile(i, 2)), x)
        return pltpu.roll(above, 1, 0), pltpu.roll(below, 7, 0)

    def loop(lo, hi, body):
        for i in range(lo, hi):
            body(i)

    def left_of(x, s):
        return pltpu.roll(x, s, 1)

    def right_of(x, s):
        return pltpu.roll(x, COLS - s, 1)

    def halved(ref, i, s):
        def at(d):
            return take(ref, pl.ds(16 * i + 8 + d, 8, stride=2))

        pair = at(0) + at(1)
        beside = jnp.where((lane & s) == 0, right_of(pair, s), left_of(pair, s))
        return 0.25 * (pair + beside)

    viscs, frics = (vx, f1, f2), (fx, res1, g2)
    for level in range(LEVELS):
        s = 1 << level
        n = tiles[level]
        kr, vr, fr = ks[level], viscs[level], frics[level]
        if level:

            def coarsen(i, level=level, vr=vr, fr=fr, s=s):
                put(vr, tile(i), halved(viscs[level - 1], i, s // 2))
                put(fr, tile(i), halved(frics[level - 1], i, s // 2))

            put(vr, slice(0, 8), zero8)
            put(vr, slice(n * 8 + 8, n * 8 + 16), zero8)
            for i in range(n):
                coarsen(i)
        scale = 0.5 * 0.25**level
        start = base >> level

        def coefficients(i, level=level, kr=kr, vr=vr, fr=fr, s=s, scale=scale, start=start):
            x = take(vr, tile(i))
            above, below = shifted(vr, i)
            cu = scale * (x + above)
            cd = scale * (x + below)
            cl = scale * (x + jnp.where(lane < s, 0.0, left_of(x, s)))
            cr = scale * (x + jnp.where(lane >= COLS - s, 0.0, right_of(x, s)))
            diag = cu + cd + cl + cr + take(fr, tile(i))
            row = start + 8 * i + rowi
            inside = (row >= 0) & (row < (COLS >> level))
            inv = jnp.where(inside, omega / diag, 0.0)
            kr[UP, tile(i), :] = inv * cu
            kr[DOWN, tile(i), :] = inv * cd
            kr[LEFT, tile(i), :] = jnp.where(lane < s, 0.0, inv * cl)
            kr[RIGHT, tile(i), :] = jnp.where(lane >= COLS - s, 0.0, inv * cr)
            kr[SCALE, tile(i), :] = jnp.where(inside, diag * (1.0 / omega), 0.0)
            kr[INV, tile(i), :] = inv
            if level == 0:
                kr[G, tile(i), :] = inv * sx[tile(i), :]

        loop(0, n, coefficients)

    def step_of(level, src, i):
        kr, s = ks[level], 1 << level
        v = src[tile(i), :]
        above, below = shifted(src, i)
        total = kr[G, tile(i), :] + kr[UP, tile(i), :] * above + kr[DOWN, tile(i), :] * below
        total = total + kr[LEFT, tile(i), :] * left_of(v, s)
        total = total + kr[RIGHT, tile(i), :] * right_of(v, s)
        return v, total - omega * v

    def core_tiles(level, h):
        n = tiles[level]
        return max(n // 3 - h, 0), min(2 * n // 3 + h, n)

    def sweep(level, a, b, h):
        src, dst = vs[level].at[a], vs[level].at[b]

        def body(i):
            v, t = step_of(level, src, i)
            dst[tile(i), :] = v + t

        loop(*core_tiles(level, h), body)

    def residual(level, a, h, res):
        src = vs[level].at[a]

        def body(i):
            _, t = step_of(level, src, i)
            put(res, tile(i), t * ks[level][SCALE, tile(i), :])

        loop(*core_tiles(level, h), body)

    def free_sweep(level, a, h, source, s):
        kr, dst = ks[level], vs[level].at[a]

        def body(i):
            if source is not None:
                kr[G, tile(i), :] = kr[INV, tile(i), :] * halved(source, i, s)
            dst[tile(i), :] = kr[G, tile(i), :]

        if source is None:
            loop(*core_tiles(level, h), body)
            return
        for i in range(*core_tiles(level, h)):
            body(i)

    def correct(level, a, b, h, spread):
        fine, coarse = vs[level].at[a], vs[level + 1].at[b]
        lo, hi = core_tiles(level, h)

        def widen(i):
            e = coarse[tile(i), :]
            put(spread, pl.ds(16 * i + 8, 8, stride=2), e)
            put(spread, pl.ds(16 * i + 9, 8, stride=2), e)

        for i in range(lo // 2, (hi + 1) // 2):
            widen(i)

        def add(i):
            fine[tile(i), :] += take(spread, tile(i))

        loop(lo, hi, add)

    def clear(ref, i):
        put(ref, tile(i, 0), zero8)

    for level in range(LEVELS):
        for a in range(2):
            loop(0, tiles[level] + 2, functools.partial(clear, vs[level].at[a]))
    loop(0, tiles[0] + 2, functools.partial(clear, res0))
    loop(0, tiles[1] + 2, functools.partial(clear, res1))

    for cycle in range(CYCLES):
        first = cycle == 0
        now = 1
        if first:
            free_sweep(0, 0, 8, None, 1)
        else:
            sweep(0, 1, 0, 4)
        sweep(0, 0, 1, 8 if first else 4)
        residual(0, now, 7 if first else 4, res0)
        free_sweep(1, 0, 4 if first else 2, res0, 1)
        sweep(1, 0, 1, 4 if first else 2)
        residual(1, 1, 3 if first else 2, res1)
        h2 = 2 if first else 1
        free_sweep(2, 0, h2, res1, 2)
        sweep(2, 0, 1, h2)
        sweep(2, 1, 0, h2)
        sweep(2, 0, 1, h2)
        correct(1, 1, 1, 3 if first else 1, f1)
        sweep(1, 1, 0, 3 if first else 1)
        sweep(1, 0, 1, 3 if first else 1)
        correct(0, now, 1, 4 if first else 1, vx)
        sweep(0, now, 1 - now, 4 if first else 1)
        sweep(0, 1 - now, now, 4 if first else 0)
    out[...] = v0[1, 72:136, :]


def solve(where, own, partner, near, visc, fric, drive, edge):
    def rows(level, *lead):
        return pltpu.VMEM((*lead, (EXT >> level) + 16, COLS), f32)

    def blocks(level):
        return pltpu.VMEM((8, (EXT >> level) + 16, 128), f32)

    return pl.pallas_call(
        solve_kernel,
        out_shape=jax.ShapeDtypeStruct((HALF, COLS), f32),
        in_specs=[SMEM] + [VMEM] * 7,
        out_specs=VMEM,
        scratch_shapes=[
            blocks(0),
            blocks(0),
            rows(0),
            rows(0, 7),
            rows(1, 7),
            rows(2, 7),
            rows(0, 2),
            rows(1, 2),
            rows(2, 2),
            blocks(1),
            rows(2),
            rows(2),
            blocks(0),
            blocks(1),
        ],
        cost_estimate=cost(10),
        name="solve",
    )(where, own, partner, near, visc, fric, drive, edge)


def flip(n, k):
    return [(i, i ^ k) for i in range(n)]


def pairs(n, turn):
    later = [(i, i + 1) for i in range(turn, n - 1, 2)]
    return later + [(b, a) for a, b in later]


def step(temp, uvel, vvel, col, cell, cav, thick, visc, fric, drive):
    core = lax.axis_index("co").astype(i32)
    y = lax.axis_index("y").astype(i32)
    blk = lax.axis_index("xh").astype(i32) * 4 + y
    where = jnp.stack([blk * CELLS, core, blk * ROWS + core * HALF - 64, y & 1])

    packet, row_a, row_b, col_a, col_b = pack(where, temp, uvel, vvel, col, cell, cav)
    got = [packet] + [lax.ppermute(packet, "y", flip(4, k)) for k in range(1, 4)]
    got = jnp.stack(got)
    away = lax.ppermute(got, "xh", flip(2, 1))

    ring = ("co", "xh", "y")
    outer = [(b, 8 + b - 1) for b in range(1, 8)] + [(8 + b, b + 1) for b in range(7)]
    ice = jnp.stack([visc, fric, drive])
    ice_edge = lax.dynamic_slice_in_dim(ice, core * HALF, HALF, axis=1)
    edge = lax.ppermute(ice_edge, ring, outer)
    row_a = lax.ppermute(row_a, "co", flip(2, 1))
    row_b = lax.ppermute(row_b, GRP, pairs(16, 1))
    col_a = lax.ppermute(col_a, "y", flip(4, 1))
    col_b = lax.ppermute(col_b, BLK, pairs(8, 1))

    mine, other, close, far = couple(where, got, away, thick)
    theirs = lax.ppermute(other, "co", flip(2, 1))
    far = lax.ppermute(far, "xh", flip(2, 1))
    part_a = mine[:32] + theirs[:32]
    part_b = mine[32:] + theirs[32:]
    ways = {"xl": flip(2, 1), "z": flip(4, 1)}
    around = [(i, 3 - i) for i in range(4)]
    part_a = part_a + lax.ppermute(part_a, "xl", ways["xl"])
    part_b = part_b + lax.ppermute(part_b, "z", ways["z"])
    part_a = part_a + lax.ppermute(part_a, "z", ways["z"])
    part_b = part_b + lax.ppermute(part_b, "z", around)
    close = close + far
    back = [lax.ppermute(close[k], "y", flip(4, k))[None] for k in range(1, 4)]
    part_a = part_a + lax.ppermute(part_a, "z", around)
    part_b = part_b + lax.ppermute(part_b, "xl", ways["xl"])
    own = jnp.concatenate([part_a, part_b], axis=0)
    partner = lax.ppermute(own, "co", flip(2, 1))
    near = lax.ppermute(own, ring, outer)
    half = solve(where, own, partner, near, visc, fric, drive, edge)
    rest = lax.ppermute(half, "co", flip(2, 1))
    temp_new = ocean(
        where, temp, uvel, vvel, row_a, row_b, col_a, col_b, col, cav, packet,
        close[0:1], *back,
    )
    first = core == 0
    ice_velocity = jnp.concatenate(
        [jnp.where(first, half, rest), jnp.where(first, rest, half)], axis=0
    )
    return temp_new, ice_velocity


def solution(mesh):
    finer = Mesh(mesh.devices.reshape(4, 2, 2, 2, 4), ("z", "xl", "co", "xh", "y"))
    field = P(None, GRP, BLK)
    entry = P(GRP, BLK, None)
    rows = P(BLK, None)
    return jax.shard_map(
        step,
        mesh=finer,
        in_specs=(field,) * 3 + (entry,) * 3 + (rows,) * 4,
        out_specs=(field, rows),
        check_vma=False,
    )
```
